128 devices in a mesh: probe: 4 (over z_hi, core), fsdp: 32 (over y, z_lo, x).
Axes of the slice: x: 4, y: 4, z: 4 (z_hi: 2, z_lo: 2; z = z_hi * 2 + z_lo), core: 2. Of those that a mesh axis runs over, the one named last changes fastest.
Arguments:
- hidden: bfloat16 [65536, 2048], P(('probe', 'fsdp')), may hold values from -6 to 6
- norm_gain: bfloat16 [2048], replicated, may hold values from 0.5 to 1.5
- query_weight: bfloat16 [2048, 2048], P('fsdp'), may hold values from -1 to 1
- key_weight: bfloat16 [2048, 512], P('fsdp'), may hold values from -16 to 16
- value_weight: bfloat16 [2048, 512], P('fsdp'), may hold values from -0.125 to 0.125
- output_weight: bfloat16 [2048, 2048], P('fsdp'), may hold values from -0.125 to 0.125
- probe_seed: int32 [4], P('probe'), may hold values from 0 to 1073741823
Outputs:
- curvature_value: float32 [2048, 512], P('fsdp', 'probe')
- curvature_output: float32 [2048, 2048], P('fsdp', 'probe')
The draws below stay inside these ranges and needn't reach their ends.
All inputs are finite; a program needn't handle non-finite values.
Results may differ from the reference program's by a relative error of at most 0.024.
Values may be sent and summed in bfloat16 or wider, within the bound.
No kernel may reach another device: no remote copies, remote signals or barrier semaphores. Data moves between devices by JAX's collectives and lax.ppermute only.
A program may use at most 128 MiB of HBM per device.

```python
import jax
import jax.numpy as jnp
from jax import lax

D = 2048
HEADS = 16
KV_HEADS = 4
HEAD_DIM = 128
SEQ = 256
TOK_DEV = 512
QW = 2048
KW = 512
TOKENS = 65536
N_PROBE = 4
N_FSDP = 32


def query_base(key):
    normals = jax.random.normal(jax.random.fold_in(key, 7101), (D, HEADS * HEAD_DIM), jnp.float32)
    return jnp.clip(normals, -6.0, 6.0) * D ** (-0.5)


def draw_query_weight(key, part):
    return query_base(key).astype(jnp.bfloat16)


def draw_key_weight(key, part):
    normals = jax.random.normal(jax.random.fold_in(key, 7102), (D, KV_HEADS * HEAD_DIM), jnp.float32)
    noise_part = jnp.clip(normals, -6.0, 6.0) * D ** (-0.5)
    return noise_part.astype(jnp.bfloat16)


def touch_ends(entries, own_key, least, largest):
    longest = entries.shape.index(max(entries.shape))
    spots = []
    for shift in (0, 1):
        where = [jax.random.randint(jax.random.fold_in(own_key, axis), (), 0, length) for axis, length in enumerate(entries.shape)]
        where[longest] = (where[longest] + shift) % entries.shape[longest]
        spots.append(tuple(where))
    return entries.at[spots[0]].set(least).at[spots[1]].set(largest)


def block_scale(stream_key, extent, split, smallest, largest):
    factor_of = 1.0
    for axis_at, blocks in split:
        draws = jax.random.uniform(jax.random.fold_in(jax.random.fold_in(stream_key, 6), axis_at), (blocks,), jnp.float32, smallest / len(split), largest / len(split))
        factor_of = factor_of * jnp.repeat(jnp.exp(draws), extent[axis_at] // blocks).reshape((-1,) + (1,) * (len(extent) - 1 - axis_at))
    return factor_of


def gaussian(stream_key, shape, scale, bound, split=(), kind=jnp.bfloat16):
    factor_of = block_scale(stream_key, shape, split, -0.22, 0.18) if split else 1.0
    values = jax.random.normal(stream_key, shape, jnp.float32) * scale * factor_of
    return jnp.minimum(jnp.maximum(values, -bound), bound).astype(kind)


def setup_inputs(seed: int = 0) -> dict:
    seeds = jax.random.split(jax.random.key(seed), 8)
    return {
        "hidden": gaussian(seeds[0], (TOKENS, D), 1.0, 6.0, ((0, 128),)),
        "norm_gain": jnp.clip(1.0 + 0.1 * jax.random.normal(seeds[1], (D,), jnp.float32), 0.5, 1.5).astype(jnp.bfloat16),
        "query_weight": draw_query_weight(jax.random.fold_in(seeds[7], 71), 0),
        "key_weight": draw_key_weight(jax.random.fold_in(seeds[7], 71), 0),
        "value_weight": gaussian(seeds[4], (D, KW), D ** -0.5, 0.125, ((0, 32),)),
        "output_weight": gaussian(seeds[5], (QW, D), QW ** -0.5, 0.125, ((0, 32),)),
        "probe_seed": touch_ends(jax.random.randint(seeds[6], (N_PROBE,), 0, 1073741824), jax.random.fold_in(seeds[6], 1), 0, 1073741823).astype(jnp.int32),
    }


norm_eps = 1e-05
rope_base = 500000.0

def sign_table(seed_value, matrix_code, row_total, column_total):
    row_index = lax.broadcasted_iota(jnp.int32, (row_total, column_total), 0)
    column_index = lax.broadcasted_iota(jnp.int32, (row_total, column_total), 1)
    hashed = (row_index * column_total + column_index) * 747796405 + (seed_value * 1664525 + matrix_code * 374761393)
    hashed = hashed ^ lax.shift_right_logical(hashed, jnp.int32(15))
    hashed = hashed * 668265261
    hashed = hashed ^ lax.shift_right_logical(hashed, jnp.int32(13))
    hashed = hashed * 1274126177
    hashed = hashed ^ lax.shift_right_logical(hashed, jnp.int32(16))
    return jnp.where(hashed & 1 == 1, 1.0, -1.0).astype(jnp.bfloat16)

def normalize(rows_in, gain_row):
    values = rows_in.astype(jnp.float32)
    inverse = lax.rsqrt(lax.optimization_barrier(jnp.mean(values * values, axis=1, keepdims=True)) + norm_eps)
    return (values * inverse * gain_row.astype(jnp.float32)[None, :]).astype(jnp.bfloat16)

def rotate(projected, head_count):
    row_count = projected.shape[0]
    columns = projected.shape[1]
    head_size = columns // head_count
    half_dim = head_size // 2
    position = (lax.broadcasted_iota(jnp.int32, (row_count, 1), 0) % SEQ).astype(jnp.float32)
    exponent = lax.broadcasted_iota(jnp.int32, (1, half_dim), 1).astype(jnp.float32) * (-2.0 / head_size)
    frequency = jnp.power(jnp.float32(rope_base), exponent)
    angles = position * frequency
    cosine = jnp.cos(angles)[:, None, :]
    sine_part = jnp.sin(angles)[:, None, :]
    shaped = projected.reshape(row_count, head_count, head_size)
    leading = shaped[:, :, :half_dim]
    trailing = shaped[:, :, half_dim:]
    turned = jnp.concatenate([leading * cosine - trailing * sine_part, trailing * cosine + leading * sine_part], axis=2)
    return turned.reshape(row_count, columns).astype(jnp.bfloat16)

def attend(query_rows, key_rows):
    row_count = query_rows.shape[0]
    key_heads = key_rows.shape[1] // HEAD_DIM
    group_size = query_rows.shape[1] // key_rows.shape[1]
    sequences = row_count // SEQ
    grouped_query = query_rows.reshape(sequences, SEQ, key_heads, group_size, HEAD_DIM).astype(jnp.float32)
    grouped_key = key_rows.reshape(sequences, SEQ, key_heads, HEAD_DIM).astype(jnp.float32)
    scores = jnp.einsum('bqkgd,bskd->bkgqs', grouped_query, grouped_key) * HEAD_DIM ** (-0.5)
    causal_mask = lax.broadcasted_iota(jnp.int32, (SEQ, SEQ), 0) >= lax.broadcasted_iota(jnp.int32, (SEQ, SEQ), 1)
    scores = jnp.where(causal_mask, scores, -1e+30)
    highest = lax.optimization_barrier(jnp.max(scores, axis=4, keepdims=True))
    raised = jnp.exp(scores - highest)
    return (raised / lax.optimization_barrier(jnp.sum(raised, axis=4, keepdims=True))).astype(jnp.bfloat16)

def mix_values(attention, value_rows):
    sequences = attention.shape[0]
    key_heads = attention.shape[1]
    group_size = attention.shape[2]
    grouped_value = value_rows.reshape(sequences, SEQ, key_heads, HEAD_DIM).astype(jnp.float32)
    combined = jnp.einsum('bkgqs,bskd->bqkgd', attention.astype(jnp.float32), grouped_value)
    return combined.reshape(sequences * SEQ, key_heads * group_size * HEAD_DIM)

def spread_back(attention, upstream):
    sequences = attention.shape[0]
    key_heads = attention.shape[1]
    group_size = attention.shape[2]
    grouped_upstream = upstream.reshape(sequences, SEQ, key_heads, group_size, HEAD_DIM).astype(jnp.float32)
    spread = jnp.einsum('bkgqs,bqkgd->bskd', attention.astype(jnp.float32), grouped_upstream)
    return spread.reshape(sequences * SEQ, key_heads * HEAD_DIM)

def device_terms(rows_in, norm_gain, query_weight, key_weight, value_weight, output_weight, seed_value):
    normed = normalize(rows_in, norm_gain)
    query_rows = rotate(jnp.dot(normed, query_weight, preferred_element_type=jnp.float32), HEADS)
    key_rows = rotate(jnp.dot(normed, key_weight, preferred_element_type=jnp.float32), KV_HEADS)
    value_rows = jnp.dot(normed, value_weight, preferred_element_type=jnp.float32).astype(jnp.bfloat16)
    attention = attend(query_rows, key_rows)
    context = mix_values(attention, value_rows).astype(jnp.bfloat16)
    signs_value = sign_table(seed_value, 0, D, KW)
    signs_out = sign_table(seed_value, 1, QW, D)
    tangent_value = (jnp.dot(normed, signs_value, preferred_element_type=jnp.float32) * D ** (-0.5)).astype(jnp.bfloat16)
    tangent_context = mix_values(attention, tangent_value).astype(jnp.bfloat16)
    forward_part = jnp.dot(tangent_context, output_weight, preferred_element_type=jnp.float32)
    probe_part = jnp.dot(context, signs_out, preferred_element_type=jnp.float32) * QW ** (-0.5)
    cotangent = (forward_part + probe_part).astype(jnp.bfloat16)
    back_context = jnp.dot(cotangent, output_weight.T, preferred_element_type=jnp.float32).astype(jnp.bfloat16)
    back_value = spread_back(attention, back_context).astype(jnp.bfloat16)
    term_value = jnp.dot(normed.T, back_value, preferred_element_type=jnp.float32)
    term_out = jnp.dot(context.T, cotangent, preferred_element_type=jnp.float32)
    return (term_value, term_out)

def reference(hidden, norm_gain, query_weight, key_weight, value_weight, output_weight, probe_seed):
    blocks = N_PROBE * N_FSDP

    def one_block(totals, block_index):
        rows_in = lax.dynamic_slice_in_dim(hidden, block_index * TOK_DEV, TOK_DEV, 0)
        seed_value = probe_seed[block_index // N_FSDP]
        term_value, term_out = device_terms(rows_in, norm_gain, query_weight, key_weight, value_weight, output_weight, seed_value)
        rounded_value = lax.optimization_barrier(term_value.astype(jnp.bfloat16))
        rounded_out = lax.optimization_barrier(term_out.astype(jnp.bfloat16))
        return ((totals[0] + rounded_value.astype(jnp.float32), totals[1] + rounded_out.astype(jnp.float32)), None)
    starting = (jnp.zeros((D, KW), jnp.float32), jnp.zeros((QW, D), jnp.float32))
    totals, unused = lax.scan(one_block, starting, jnp.arange(blocks, dtype=jnp.int32))
    return (totals[0], totals[1])
```

```python
import functools

import jax
import jax.numpy as jnp
from jax import lax
from jax.experimental import pallas as pl
from jax.experimental.pallas import tpu as pltpu
from jax.sharding import Mesh
from jax.sharding import PartitionSpec as P

HEAD_DIM = 128
SEQ = 256


norm_eps = 1e-05
rope_base = 500000.0


AXES = ("zh", "core", "y", "zl", "x")
Z = ("zh", "zl")


def shifted(value, axis, by):
    size = lax.axis_size(axis)
    return lax.ppermute(value, axis, [(i, (i + by) % size) for i in range(size)])


def gather_kernel(plan, place, *refs):
    sems = refs[-1]
    copies = [
        pltpu.make_async_copy(src, dst, sems.at[k])
        for k, (src, dst) in enumerate(plan(place, refs[:-1]))
    ]
    for c in copies:
        c.start()
    for c in copies:
        c.wait()


def placed(name, plan, count, place, pieces, shapes):
    return pl.pallas_call(
        functools.partial(gather_kernel, plan),
        in_specs=[pl.BlockSpec(memory_space=pltpu.SMEM)]
        + [pl.BlockSpec(memory_space=pl.ANY)] * len(pieces),
        out_specs=[pl.BlockSpec(memory_space=pl.ANY)] * len(shapes),
        out_shape=[jax.ShapeDtypeStruct(s, jnp.bfloat16) for s in shapes],
        scratch_shapes=[pltpu.SemaphoreType.DMA((count,))],
        name=name,
    )(place, *pieces)


def small_plan(axis_at, place, refs):
    own, before, after, across, first, second = refs
    at = place[axis_at]
    split = first.shape[-1]
    pairs = []
    for piece, by in ((own, 0), (before, 3), (after, 1), (across, 2)):
        slot = lax.rem(at + by, 4)
        for out, cols in ((first, pl.ds(0, split)), (second, pl.ds(split, second.shape[-1]))):
            target = out.at[:, slot] if axis_at == 3 else out.at[slot]
            pairs.append((piece.at[:, :, cols], target))
    return pairs


def large_plan(place, refs):
    a, b, (out_a, out_b) = refs[:5], refs[5:10], refs[10:]
    y, x = place[1], place[3]
    pairs = []
    for piece, by in ((a[0], 0), (a[1], 3), (a[2], 1)):
        pairs.append((piece, out_a.at[lax.rem(y + by, 4)]))
    for k in range(2):
        pairs.append((a[3 + k], out_a.at[lax.rem(y + 2, 4), pl.ds(k, 1)]))
    for piece, by in ((b[0], 0), (b[1], 3), (b[2], 1)):
        pairs.append((piece, out_b.at[:, :, lax.rem(x + by, 4)]))
    for k in range(2):
        pairs.append((b[3 + k], out_b.at[pl.ds(2 * k, 2), :, lax.rem(x + 2, 4)]))
    return pairs


def line_of(value, axis):
    return value, shifted(value, axis, 1), shifted(value, axis, -1), shifted(value, axis, 2)


def passed_on(value, axis, half):
    before, after = shifted(value, axis, 1), shifted(value, axis, -1)
    return (
        value,
        before,
        after,
        shifted(before[0:half], axis, 1),
        shifted(after[half:], axis, -1),
    )


def gathered(place, shard, split):
    zl = place[2]
    low, high = shifted(shard[:32], Z, -1), shifted(shard[32:], Z, 1)
    other = jnp.concatenate([low, high], 0)
    both = jnp.where(zl == 0, jnp.stack([shard, other]), jnp.stack([other, shard]))
    half, rest = split // 2, (shard.shape[1] - split) // 2
    a = jnp.concatenate([both[:, :, :half], both[:, :, split : split + rest]], 2)
    b = jnp.concatenate([both[:, :, half:split], both[:, :, split + rest :]], 2)
    a_first, a_second = placed(
        "small_a", functools.partial(small_plan, 3), 8, place, line_of(a, "x"),
        [(2, 4, 64, half), (2, 4, 64, rest)],
    )
    b_first, b_second = placed(
        "small_b", functools.partial(small_plan, 1), 8, place, line_of(b, "y"),
        [(4, 2, 64, half), (4, 2, 64, rest)],
    )
    results = []
    for name, pa, pb, cols in (("first", a_first, b_first, half), ("second", a_second, b_second, rest)):
        wa, wb = placed(
            "large_" + name, large_plan, 10, place,
            passed_on(pa, "y", 1) + passed_on(pb, "x", 2),
            [(4, 2, 4, 64, cols)] * 2,
        )
        wa, wb = wa.reshape(2048, cols), wb.reshape(2048, cols)
        results.append((wa, wb, shifted(wa, "core", 1), shifted(wb, "core", 1)))
    return results


def summed_line(value, axis, at, dim, dtype):
    pick = lambda by: lax.dynamic_index_in_dim(value, (at + by) % 4, dim, keepdims=False)
    total = pick(0).astype(jnp.float32)
    for by in (1, 3, 2):
        total += shifted(pick(by), axis, by).astype(jnp.float32)
    return total.astype(dtype)


def scattered(place, own, partner):
    y, x = place[1], place[3]
    z = 2 * place[4] + place[2]
    both = (own.astype(jnp.float32) + shifted(partner, "core", 1).astype(jnp.float32)).astype(jnp.bfloat16)
    both = both.reshape(4, 2, 4, 64, 1280)
    a = summed_line(both[:, :, :, :32], "x", x, 2, jnp.bfloat16)
    b = summed_line(both[:, :, :, 32:], "y", y, 0, jnp.bfloat16)
    a = summed_line(a, "y", y, 0, jnp.bfloat16)
    b = summed_line(b, "x", x, 1, jnp.bfloat16)
    last = jnp.concatenate([a, b], 1).reshape(2, 64, 2, 640)
    last = jnp.moveaxis(last, 2, 0).reshape(4, 64, 640)
    return summed_line(last, Z, z, 0, jnp.float32)

def sign_table(seed_value, matrix_code, row_total, column_total, first, width):
    row_index = lax.broadcasted_iota(jnp.int32, (row_total, width), 0)
    column_index = lax.broadcasted_iota(jnp.int32, (row_total, width), 1) + first
    hashed = (row_index * column_total + column_index) * 747796405 + (
        seed_value * 1664525 + matrix_code * 374761393
    )
    hashed = hashed ^ lax.shift_right_logical(hashed, jnp.int32(15))
    hashed = hashed * 668265261
    hashed = hashed ^ lax.shift_right_logical(hashed, jnp.int32(13))
    hashed = hashed * 1274126177
    hashed = hashed ^ lax.shift_right_logical(hashed, jnp.int32(16))
    return jnp.where(hashed & 1 == 1, 1.0, -1.0).astype(jnp.bfloat16)


def normalize(rows_in, gain_row):
    values = rows_in.astype(jnp.float32)
    inverse = lax.rsqrt(jnp.mean(values * values, axis=1, keepdims=True) + norm_eps)
    return (values * inverse * gain_row.astype(jnp.float32)[None, :]).astype(jnp.bfloat16)


def rotate(projected, head_count):
    row_count = projected.shape[0]
    columns = projected.shape[1]
    head_size = columns // head_count
    half_dim = head_size // 2
    position = (lax.broadcasted_iota(jnp.int32, (row_count, 1), 0) % SEQ).astype(jnp.float32)
    exponent = lax.broadcasted_iota(jnp.int32, (1, half_dim), 1).astype(jnp.float32) * (
        -2.0 / head_size
    )
    frequency = jnp.power(jnp.float32(rope_base), exponent)
    angles = position * frequency
    cosine = jnp.cos(angles)[:, None, :]
    sine_part = jnp.sin(angles)[:, None, :]
    shaped = projected.reshape(row_count, head_count, head_size)
    leading = shaped[:, :, :half_dim]
    trailing = shaped[:, :, half_dim:]
    turned = jnp.concatenate(
        [leading * cosine - trailing * sine_part, trailing * cosine + leading * sine_part], axis=2
    )
    return turned.reshape(row_count, columns).astype(jnp.bfloat16)


def attend(query_rows, key_rows):
    row_count = query_rows.shape[0]
    key_heads = key_rows.shape[1] // HEAD_DIM
    group_size = query_rows.shape[1] // key_rows.shape[1]
    sequences = row_count // SEQ
    grouped_query = query_rows.reshape(sequences, SEQ, key_heads, group_size, HEAD_DIM)
    grouped_key = key_rows.reshape(sequences, SEQ, key_heads, HEAD_DIM)
    scores = jnp.einsum(
        "bqkgd,bskd->bkgqs", grouped_query, grouped_key, preferred_element_type=jnp.float32
    ) * HEAD_DIM ** (-0.5)
    causal_mask = lax.broadcasted_iota(jnp.int32, (SEQ, SEQ), 0) >= lax.broadcasted_iota(
        jnp.int32, (SEQ, SEQ), 1
    )
    scores = jnp.where(causal_mask, scores, -1e30)
    highest = jnp.max(scores, axis=4, keepdims=True)
    raised = jnp.exp(scores - highest)
    return (raised / jnp.sum(raised, axis=4, keepdims=True)).astype(jnp.bfloat16)


def mix_values(attention, value_rows):
    sequences = attention.shape[0]
    key_heads = attention.shape[1]
    group_size = attention.shape[2]
    grouped_value = value_rows.reshape(sequences, SEQ, key_heads, HEAD_DIM)
    combined = jnp.einsum(
        "bkgqs,bskd->bqkgd", attention, grouped_value, preferred_element_type=jnp.float32
    )
    return combined.reshape(sequences * SEQ, key_heads * group_size * HEAD_DIM)


def spread_back(attention, upstream):
    sequences = attention.shape[0]
    key_heads = attention.shape[1]
    group_size = attention.shape[2]
    grouped_upstream = upstream.reshape(sequences, SEQ, key_heads, group_size, HEAD_DIM)
    spread = jnp.einsum(
        "bkgqs,bqkgd->bskd", attention, grouped_upstream, preferred_element_type=jnp.float32
    )
    return spread.reshape(sequences * SEQ, key_heads * HEAD_DIM)


def body(hidden, norm_gain, query_weight, key_weight, value_weight, output_weight, probe_seed):
    seed_value = probe_seed[0]
    zh, core = lax.axis_index("zh"), lax.axis_index("core")
    y, zl, x = (lax.axis_index(a) for a in ("y", "zl", "x"))
    place = jnp.stack([core, y, zl, x, zh]).astype(jnp.int32)
    cut = lambda w, n: lax.dynamic_slice_in_dim(w, core * n, n, 1)
    quarter = lambda p: lax.dynamic_slice_in_dim(output_weight, p * 512, 512, 1)
    shard = jnp.concatenate(
        [cut(query_weight, 1024), cut(key_weight, 256), cut(value_weight, 256), quarter(core), quarter(2 + core)], 1
    )
    projections, outputs = gathered(place, shard, 1536)
    normed = normalize(hidden, norm_gain)
    dot = functools.partial(jnp.dot, preferred_element_type=jnp.float32)
    ordered = lambda own, partner: jnp.where(
        core == 0, jnp.concatenate([own, partner], 1), jnp.concatenate([partner, own], 1)
    )
    raw = [dot(normed, w) for w in projections]
    query_raw = ordered(
        jnp.concatenate([raw[0], raw[1][:, :256]], 1), jnp.concatenate([raw[2], raw[3][:, :256]], 1)
    )
    key_raw = ordered(raw[1][:, 256:512], raw[3][:, 256:512])
    value_raw = ordered(raw[1][:, 512:], raw[3][:, 512:])
    query_rows = rotate(query_raw, 16)
    key_rows = rotate(key_raw, 4)
    value_rows = value_raw.astype(jnp.bfloat16)
    attention = attend(query_rows, key_rows)
    context = mix_values(attention, value_rows).astype(jnp.bfloat16)
    signs_value = sign_table(seed_value, 0, 2048, 512, 0, 512)
    tangent_value = (dot(normed, signs_value) * 2048 ** (-0.5)).astype(jnp.bfloat16)
    tangent_context = mix_values(attention, tangent_value).astype(jnp.bfloat16)
    quarters = [core, 2 + core, 1 - core, 3 - core]
    cotangent, back_context = [], 0.0
    for w, p in zip(outputs, quarters):
        signs = sign_table(seed_value, 1, 2048, 2048, p * 512, 512)
        part = (dot(tangent_context, w) + dot(context, signs) * 2048 ** (-0.5)).astype(jnp.bfloat16)
        cotangent.append(part)
        back_context += lax.dot_general(part, w, (((1,), (1,)), ((), ())), preferred_element_type=jnp.float32)
    back_value = spread_back(attention, back_context.astype(jnp.bfloat16)).astype(jnp.bfloat16)
    rows = (((0,), (0,)), ((), ()))
    terms = []
    for part, p in zip(cotangent, quarters):
        columns = lax.dynamic_slice_in_dim(back_value, p * 128, 128, 1)
        terms.append(lax.dot_general(context, part, rows, preferred_element_type=jnp.float32).astype(jnp.bfloat16))
        terms.append(lax.dot_general(normed, columns, rows, preferred_element_type=jnp.float32).astype(jnp.bfloat16))
    own, partner = jnp.concatenate(terms[:4], 1), jnp.concatenate(terms[4:], 1)
    result = scattered(place, own, partner)
    return result[:, 512:], result[:, :512]


def solution(mesh):
    fine = Mesh(mesh.devices.reshape(2, 2, 4, 2, 4), AXES)
    fsdp, probe = ("y", "zl", "x"), ("zh", "core")
    return jax.shard_map(
        body,
        mesh=fine,
        in_specs=(P(AXES, None), P(), P(fsdp, None), P(fsdp, None), P(fsdp, None), P(fsdp, None), P(probe)),
        out_specs=(P(fsdp, probe), P(fsdp, probe)),
        check_vma=False,
    )
```

```python
import functools

import jax
import jax.numpy as jnp
from jax import lax
from jax.experimental import pallas as pl
from jax.experimental.pallas import tpu as pltpu
from jax.sharding import Mesh
from jax.sharding import PartitionSpec as P

HEAD_DIM = 128
SEQ = 256
AXES = ("zh", "core", "y", "zl", "x")
Z = ("zh", "zl")
norm_eps = 1e-05
rope_base = 500000.0
bf16, f32 = jnp.bfloat16, jnp.float32
ROWS = (((0,), (0,)), ((), ()))
LAST = (((1,), (1,)), ((), ()))


def dot(a, b):
    return jnp.dot(a, b, preferred_element_type=f32)


def call(name, kernel, place, args, shapes, scratch=(), flops=0, anywhere=(), dtypes=None):
    dtypes = dtypes or [bf16] * len(shapes)
    specs = [pl.BlockSpec(memory_space=pltpu.SMEM)]
    for i in range(len(args)):
        specs.append(pl.BlockSpec(memory_space=pl.ANY if i in anywhere else pltpu.VMEM))
    moved = sum(a.size * a.dtype.itemsize for a in args)
    return pl.pallas_call(
        kernel,
        in_specs=specs,
        out_specs=[pl.BlockSpec(memory_space=pltpu.VMEM)] * len(shapes),
        out_shape=[jax.ShapeDtypeStruct(s, d) for s, d in zip(shapes, dtypes)],
        scratch_shapes=list(scratch),
        compiler_params=pltpu.CompilerParams(vmem_limit_bytes=60 * 1024 * 1024),
        cost_estimate=pl.CostEstimate(flops=flops or moved // 2, bytes_accessed=moved, transcendentals=0),
        name=name,
    )(place, *args)


def shifted(value, axis, by):
    size = lax.axis_size(axis)
    return lax.ppermute(value, axis, [(i, (i + by) % size) for i in range(size)])


def line_of(value, axis):
    return value, shifted(value, axis, 1), shifted(value, axis, -1), shifted(value, axis, 2)


def passed_on(value, axis, half):
    before, after = shifted(value, axis, 1), shifted(value, axis, -1)
    return (
        value,
        before,
        after,
        shifted(before[0:half], axis, 1),
        shifted(after[half:], axis, -1),
    )


def local_slot(y, core):
    return lax.div(y, 2) + 2 * lax.rem(lax.rem(y, 2) + core, 2)


def cut_kernel(place, q, k, v, o, low, high):
    core = place[0]
    for color in range(2):
        p = 2 * color + core
        at = 1280 * color
        for ref, width, to in ((q, 512, 0), (k, 128, 512), (v, 128, 640), (o, 512, 768)):
            cols = pl.ds(pl.multiple_of(p * width, width), width)
            low[:, at + to : at + to + width] = ref[0:32, cols]
            high[:, at + to : at + to + width] = ref[32:64, cols]


def join_kernel(place, low, high, other_low, other_high, a, b):
    zl = place[2]
    for slot, parts in ((zl, (low, high)), (1 - zl, (other_low, other_high))):
        for color, out in enumerate((a, b)):
            cols = slice(1280 * color, 1280 * color + 1280)
            out[slot, 0:32] = parts[0][:, cols]
            out[slot, 32:64] = parts[1][:, cols]


def small_kernel(along_x, place, own, before, after, across, first, second):
    core, y, x = place[0], place[1], place[3]
    for piece, by in ((own, 0), (before, 3), (after, 1), (across, 2)):
        if along_x:
            slot = lax.rem(x + by, 4)
            first[:, slot] = piece[:, :, :768]
            second[:, slot] = piece[:, :, 768:]
        else:
            slot = lax.rem(y + by, 4)
            first[slot] = piece[:, :, :768]
            second[local_slot(slot, core)] = piece[:, :, 768:]


def large_kernel(local, place, *refs):
    a, b, out, sems = refs[:5], refs[5:10], refs[10], refs[11]
    core, y, x = place[0], place[1], place[3]
    row = (lambda v: local_slot(lax.rem(v, 4), core)) if local else (lambda v: lax.rem(v, 4))
    pairs = []
    for piece, by in ((a[0], 0), (a[1], 3), (a[2], 1)):
        pairs.append((piece, out.at[0, row(y + by)]))
    for k in range(2):
        pairs.append((a[3 + k], out.at[0, row(y + 2), pl.ds(k, 1)]))
    for piece, by in ((b[0], 0), (b[1], 3), (b[2], 1)):
        pairs.append((piece, out.at[1, :, :, lax.rem(x + by, 4)]))
    for k in range(2):
        pairs.append((b[3 + k], out.at[1, pl.ds(2 * k, 2), :, lax.rem(x + 2, 4)]))
    copies = [pltpu.make_async_copy(s, d, sems.at[i]) for i, (s, d) in enumerate(pairs)]
    for c in copies:
        c.start()
    for c in copies:
        c.wait()


def hashed_signs(index, seed_term):
    h = index * 747796405 + seed_term
    h = h ^ lax.shift_right_logical(h, jnp.int32(15))
    h = h * 668265261
    h = h ^ lax.shift_right_logical(h, jnp.int32(13))
    h = h * 1274126177
    h = h ^ lax.shift_right_logical(h, jnp.int32(16))
    return jnp.where(h & 1 == 1, 1.0, -1.0).astype(bf16)


def local_quarter(core, j):
    return lax.rem(core + lax.div(j, 2), 2) + 2 * lax.rem(j, 2)


def signs_kernel(place, out):
    core, j = place[0], pl.program_id(0)
    rows, cols = local_quarter(core, lax.div(j, 4)) * 512, local_quarter(core, lax.rem(j, 4)) * 512
    seed_term = place[5] * 1664525 + 374761393
    r = lax.broadcasted_iota(jnp.int32, (512, 512), 0) + rows
    s = lax.broadcasted_iota(jnp.int32, (512, 512), 1) + cols
    out[...] = hashed_signs(r * 2048 + s, seed_term)


def sign_table(place):
    return pl.pallas_call(
        signs_kernel,
        grid=(16,),
        in_specs=[pl.BlockSpec(memory_space=pltpu.SMEM)],
        out_specs=pl.BlockSpec((512, 512), lambda j: (j // 4, j % 4)),
        out_shape=jax.ShapeDtypeStruct((2048, 2048), bf16),
        cost_estimate=pl.CostEstimate(flops=1 << 33, bytes_accessed=1 << 23, transcendentals=0),
        name="signs",
    )(place)


def attention_kernel(place, n, w, tv, cos, sin, ctx, tctx, p_out, qkv):
    turn = lambda v: v * cos[0:SEQ] + pltpu.roll(v, 64, 1) * sin[0:SEQ]
    over = lax.broadcasted_iota(jnp.int32, (4 * SEQ, SEQ), 0) % SEQ >= lax.broadcasted_iota(
        jnp.int32, (4 * SEQ, SEQ), 1
    )
    for k in range(2):
        qkv[...] = dot(n[...], w[k])
        for s in range(2):
            rows = slice(SEQ * s, SEQ * s + SEQ)
            key = turn(qkv[rows, 512:640]).astype(bf16)
            q4 = jnp.concatenate([turn(qkv[rows, 128 * h : 128 * h + 128]).astype(bf16) for h in range(4)], 0)
            scores = lax.dot_general(q4, key, LAST, preferred_element_type=f32)
            scores = jnp.where(over, scores * HEAD_DIM ** (-0.5), -1e30)
            raised = jnp.exp(scores - jnp.max(scores, 1, keepdims=True))
            weights = (raised * (1.0 / jnp.sum(raised, 1, keepdims=True))).astype(bf16)
            p_out[s, k] = weights
            both = jnp.concatenate([qkv[rows, 640:768].astype(bf16), tv[rows, 128 * k : 128 * k + 128]], 1)
            mixed = dot(weights, both).astype(bf16)
            for h in range(4):
                to = slice(512 * k + 128 * h, 512 * k + 128 * h + 128)
                ctx[rows, to] = mixed[SEQ * h : SEQ * h + SEQ, :128]
                tctx[rows, to] = mixed[SEQ * h : SEQ * h + SEQ, 128:]


def probe_kernel(place, ctx_own, ctx_partner, signs, out):
    out[...] = (dot(ctx_own[...], signs[0:1024]) + dot(ctx_partner[...], signs[1024:2048])) * 2048 ** (-0.5)


def cotangent_kernel(at, place, c0, c1, t0, t1, w, part, *refs):
    back_in, (term, back), cot = refs[:-3], refs[-3:-1], refs[-1]
    for k in range(2):
        cols = slice(512 * k, 512 * k + 512)
        value = dot(t0[...], w[k, 0:1024]) + dot(t1[...], w[k, 1024:2048])
        cot[:, cols] = (value + part[:, at + 512 * k : at + 512 * k + 512]).astype(bf16)
    for j, c in enumerate((c0, c1)):
        term[1024 * j : 1024 * j + 1024] = lax.dot_general(
            c[...], cot[...], ROWS, preferred_element_type=f32
        ).astype(bf16)
    for j in range(2):
        rows = slice(1024 * j, 1024 * j + 1024)
        value = lax.dot_general(cot[:, 0:512], w[0, rows], LAST, preferred_element_type=f32) + lax.dot_general(
            cot[:, 512:1024], w[1, rows], LAST, preferred_element_type=f32
        )
        if back_in:
            there = slice(1024 * (1 - j), 1024 * (1 - j) + 1024)
            back[:, there] = (value + back_in[0][:, there]).astype(back.dtype)
        else:
            back[:, rows] = value


def value_kernel(place, n, p_own, p_partner, back, own, partner, bv):
    for half, p in enumerate((p_own, p_partner)):
        for k in range(2):
            for s in range(2):
                rows = slice(SEQ * s, SEQ * s + SEQ)
                at = 1024 * half + 512 * k
                up = jnp.concatenate([back[rows, at + 128 * h : at + 128 * h + 128] for h in range(4)], 0)
                to = 256 * half + 128 * k
                bv[rows, to : to + 128] = lax.dot_general(
                    p[s, k], up, ROWS, preferred_element_type=f32
                ).astype(bf16)
    term = lax.dot_general(n[...], bv[...], ROWS, preferred_element_type=f32).astype(bf16)
    own[...] = term[:, :256]
    partner[...] = term[:, 256:]


def pair_kernel(place, out_own, out_got, val_own, val_got, *pieces):
    core, y, x = place[0], place[1], place[3]
    a, b = pieces[:4], pieces[4:]
    add = lambda u, v: (u.astype(f32) + v.astype(f32)).astype(bf16)
    for by in range(4):
        slot = lax.rem(x + by, 4)
        for row in range(4):
            mine = local_slot(jnp.int32(row), core)
            a[by][row, :, :, 0:1024] = add(out_own[mine, :, slot, 0:32], out_got[mine, :, slot, 0:32])
            a[by][row, :, :, 1024:1280] = add(val_own[row, :, slot, 0:32], val_got[row, :, slot, 0:32])
        row = lax.rem(y + by, 4)
        mine = local_slot(row, core)
        b[by][:, :, :, 0:1024] = add(out_own[mine, :, :, 32:64], out_got[mine, :, :, 32:64])
        b[by][:, :, :, 1024:1280] = add(val_own[row, :, :, 32:64], val_got[row, :, :, 32:64])


def total_of(refs, index=()):
    total = refs[0][index].astype(f32)
    for r in refs[1:]:
        total += r[index].astype(f32)
    return total


def second_kernel(place, *refs):
    y, x = place[1], place[3]
    a, b, (out_a, out_b) = refs[:4], refs[4:8], (refs[8:12], refs[12:16])
    for by in range(4):
        out_a[by][...] = total_of(a, lax.rem(y + by, 4)).astype(bf16)
        slot = lax.rem(x + by, 4)
        for zl in range(2):
            out_b[by][zl] = total_of(b, (zl, slot)).astype(bf16)


def third_kernel(place, *refs):
    z = 2 * place[4] + place[2]
    a, b, out = refs[:4], refs[4:8], refs[8:]
    for by in range(4):
        to = lax.rem(z + by, 4)
        zl, zh = lax.rem(to, 2), lax.div(to, 2)
        for rows, parts in ((slice(0, 32), a), (slice(32, 64), b)):
            lo = total_of(parts, zl)
            for at, width in ((0, 512), (1024, 128)):
                left, right = lo[:, at : at + width], lo[:, at + width : at + 2 * width]
                got = jnp.where(zh == 0, left, right).astype(bf16)
                start = 0 if at == 0 else 512
                out[by][rows, start : start + width] = got


def last_kernel(place, own, before, after, across, value, output):
    total = total_of((own, before, after, across), slice(None))
    output[...] = total[:, :512]
    value[...] = total[:, 512:]


def exchanged(pieces, axis):
    return (pieces[0],) + tuple(shifted(pieces[by], axis, by) for by in (1, 3, 2))


def normalize(rows_in, gain_row):
    values = rows_in.astype(f32)
    inverse = lax.rsqrt(jnp.mean(values * values, axis=1, keepdims=True) + norm_eps)
    return (values * inverse * gain_row.astype(f32)[None, :]).astype(bf16)


def turn_tables():
    position = lax.broadcasted_iota(jnp.int32, (SEQ, 1), 0).astype(f32)
    exponent = lax.broadcasted_iota(jnp.int32, (1, 64), 1).astype(f32) * (-2.0 / HEAD_DIM)
    angles = position * jnp.power(f32(rope_base), exponent)
    cos, sin = jnp.cos(angles), jnp.sin(angles)
    return jnp.concatenate([cos, cos], 1), jnp.concatenate([-sin, sin], 1)


def body(hidden, norm_gain, query_weight, key_weight, value_weight, output_weight, probe_seed):
    seed_value = probe_seed[0]
    zh, core, y, zl, x = (lax.axis_index(a) for a in AXES)
    place = jnp.stack([core, y, zl, x, zh, seed_value]).astype(jnp.int32)

    low, high = call(
        "cut", cut_kernel, place, (query_weight, key_weight, value_weight, output_weight), [(32, 2560)] * 2
    )
    a, b = call(
        "join", join_kernel, place, (low, high, shifted(low, Z, -1), shifted(high, Z, 1)), [(2, 64, 1280)] * 2
    )
    a_first, a_second = call(
        "small_a", functools.partial(small_kernel, True), place, line_of(a, "x"), [(2, 4, 64, 768), (2, 4, 64, 512)]
    )
    b_first, b_second = call(
        "small_b", functools.partial(small_kernel, False), place, line_of(b, "y"), [(4, 2, 64, 768), (4, 2, 64, 512)]
    )
    sems = [pltpu.SemaphoreType.DMA((10,))]
    (w_own,) = call(
        "large_first", functools.partial(large_kernel, False), place,
        passed_on(a_first, "y", 1) + passed_on(b_first, "x", 2),
        [(2, 4, 2, 4, 64, 768)], sems, anywhere=range(10),
    )
    w_own = w_own.reshape(2, 2048, 768)
    w_partner = shifted(w_own, "core", 1)
    (o_own,) = call(
        "large_second", functools.partial(large_kernel, True), place,
        passed_on(a_second, "y", 1) + passed_on(b_second, "x", 2),
        [(2, 4, 2, 4, 64, 512)], sems, anywhere=range(10),
    )
    o_own = o_own.reshape(2, 2048, 512)
    o_partner = shifted(o_own, "core", 1)

    normed = normalize(hidden, norm_gain)
    cos, sin = turn_tables()
    column = lax.broadcasted_iota(jnp.int32, (1, 512), 1)
    column = local_quarter(core, column // 128) * 128 + column % 128
    row = lax.broadcasted_iota(jnp.int32, (2048, 1), 0)
    signs_value = hashed_signs(row * 512 + column, seed_value * 1664525)
    tangent_value = (dot(normed, signs_value) * 2048 ** (-0.5)).astype(bf16)
    signs = sign_table(place)

    def attend(w, tv, name):
        return call(
            name, attention_kernel, place, (normed, w, tv, cos, sin),
            [(512, 1024), (512, 1024), (2, 2, 1024, 256)], [pltpu.VMEM((512, 768), f32)], flops=5 << 30,
        )

    c_own, t_own, p_own = attend(w_own, tangent_value[:, :256], "attend_own")
    c_partner, t_partner, p_partner = attend(w_partner, tangent_value[:, 256:], "attend_partner")
    (part,) = call(
        "probe_part", probe_kernel, place, (c_own, c_partner, signs), [(512, 2048)], flops=4 << 30, dtypes=[f32]
    )
    scratch = [pltpu.VMEM((512, 1024), bf16)]
    term_own, back = call(
        "cotangent_own", functools.partial(cotangent_kernel, 0), place,
        (c_own, c_partner, t_own, t_partner, o_own, part),
        [(2048, 1024), (512, 2048)], scratch, flops=6 << 30, dtypes=[bf16, f32],
    )
    term_partner, back = call(
        "cotangent_partner", functools.partial(cotangent_kernel, 1024), place,
        (c_partner, c_own, t_partner, t_own, o_partner, part, back),
        [(2048, 1024), (512, 2048)], scratch, flops=6 << 30,
    )
    term_got = shifted(term_partner, "core", 1)
    val_own, val_partner = call(
        "value_terms", value_kernel, place, (normed, p_own, p_partner, back),
        [(2048, 256)] * 2, [pltpu.VMEM((512, 512), bf16)], flops=2 << 30,
    )
    val_got = shifted(val_partner, "core", 1)
    grid = lambda v: v.reshape(4, 2, 4, 64, v.shape[1])
    pieces = call(
        "pair", pair_kernel, place, (grid(term_own), grid(term_got), grid(val_own), grid(val_got)),
        [(4, 2, 32, 1280)] * 4 + [(2, 4, 32, 1280)] * 4,
    )
    pieces = call(
        "second", second_kernel, place, exchanged(pieces[:4], "x") + exchanged(pieces[4:], "y"),
        [(2, 32, 1280)] * 8,
    )
    pieces = call(
        "third", third_kernel, place, exchanged(pieces[:4], "y") + exchanged(pieces[4:], "x"), [(64, 640)] * 4
    )
    value, output = call(
        "last", last_kernel, place, exchanged(pieces, Z), [(64, 128), (64, 512)], dtypes=[f32, f32]
    )
    return value, output


def solution(mesh):
    fine = Mesh(mesh.devices.reshape(2, 2, 4, 2, 4), AXES)
    fsdp, probe = ("y", "zl", "x"), ("zh", "core")
    return jax.shard_map(
        body,
        mesh=fine,
        in_specs=(P(AXES, None), P(), P(fsdp, None), P(fsdp, None), P(fsdp, None), P(fsdp, None), P(probe)),
        out_specs=(P(fsdp, probe), P(fsdp, probe)),
        check_vma=False,
    )
```

```python
import functools

import jax
import jax.numpy as jnp
from jax import lax
from jax.experimental import pallas as pl
from jax.experimental.pallas import tpu as pltpu
from jax.sharding import Mesh
from jax.sharding import PartitionSpec as P

HEAD_DIM = 128
SEQ = 256
AXES = ("zh", "core", "y", "zl", "x")
Z = ("zh", "zl")
norm_eps = 1e-05
rope_base = 500000.0
LIMITS = (14, 8, 12, 10, 6)
bf16, f32 = jnp.bfloat16, jnp.float32
ROWS = (((0,), (0,)), ((), ()))
LAST = (((1,), (1,)), ((), ()))


def dot(a, b):
    return jnp.dot(a, b, preferred_element_type=f32)


def position(seed=None):
    core, y, zl, x, zh = (lax.axis_index(a) for a in ("core", "y", "zl", "x", "zh"))
    return core, y, zl, x, zh, None if seed is None else seed[0]


def call(kernel, args, shapes, scratch=(), flops=0, kept=(), far=(), dtypes=None, limit=56, seed=None):
    dtypes = dtypes or [bf16] * len(shapes)
    space = lambda i, there: pl.BlockSpec(memory_space=pltpu.HBM if i in there else pltpu.VMEM)
    moved = sum(a.size * a.dtype.itemsize for a in args)
    in_specs = [space(i, kept) for i in range(len(args))]
    if seed is None:
        run = lambda *refs: kernel(position(), *refs)
    else:
        in_specs, args = [pl.BlockSpec(memory_space=pltpu.SMEM)] + in_specs, (seed,) + tuple(args)
        run = lambda ref, *refs: kernel(position(ref), *refs)
    return pl.pallas_call(
        run,
        in_specs=in_specs,
        out_specs=[space(i, far) for i in range(len(shapes))],
        out_shape=[jax.ShapeDtypeStruct(s, d) for s, d in zip(shapes, dtypes)],
        scratch_shapes=list(scratch),
        compiler_params=pltpu.CompilerParams(vmem_limit_bytes=limit * 1024 * 1024),
        cost_estimate=pl.CostEstimate(flops=flops or moved // 2, bytes_accessed=moved, transcendentals=0),
    )(*args)


class Copies:
    def __init__(self, sems):
        self.sems, self.used, self.open = sems, 0, []

    def start(self, source, target, late=False):
        copy = pltpu.make_async_copy(source, target, self.sems.at[self.used])
        self.used += 1
        copy.start()
        if late:
            self.open.append(copy)
        return copy

    def finish(self):
        for copy in self.open:
            copy.wait()


def dma(count):
    return pltpu.SemaphoreType.DMA((count,))


def shifted(value, axis, by):
    size = lax.axis_size(axis)
    return lax.ppermute(value, axis, [(i, (i + by) % size) for i in range(size)])


def line_of(value, axis):
    return (value,) + tuple(shifted(value, axis, by) for by in (1, -1, 2))


def local_slot(y, core):
    return lax.div(y, 2) + 2 * lax.rem(lax.rem(y, 2) + core, 2)


def cut_kernel(place, q, k, v, o, a, b, sems):
    copies = Copies(sems)
    for color, out in enumerate((a, b)):
        p = 2 * color + place[0]
        for ref, width, to in ((q, 512, 0), (k, 128, 512), (v, 128, 640), (o, 512, 768)):
            cols = pl.ds(pl.multiple_of(p * width, width), width)
            copies.start(ref.at[:, cols], out.at[:, pl.ds(to, width)], True)
    copies.finish()


def small_kernel(place, *refs):
    aq, ao, bq, bo, low_q, high_q, low_o, high_o = refs[8:]
    core, y, _, x = place[:4]
    for k, by in enumerate((0, 3, 1, 2)):
        slot = lax.rem(x + by, 4)
        aq[slot] = refs[k][:, :768]
        ao[slot] = refs[k][:, 768:]
        slot = lax.rem(y + by, 4)
        bq[slot] = refs[4 + k][:, :768]
        bo[local_slot(slot, core)] = refs[4 + k][:, 768:]
    for low, high, a, b in ((low_q, high_q, aq, bq), (low_o, high_o, ao, bo)):
        for out, half in ((low, slice(0, 2)), (high, slice(2, 4))):
            out[0:2] = a[half]
            out[2:4] = b[half]


def join_kernel(place, a, b, low, high, out_a, out_b):
    zl = place[2]
    for own, out, at in ((a, out_a, 0), (b, out_b, 2)):
        out[zl] = own[...]
        out[1 - zl, 0:2] = low[at : at + 2]
        out[1 - zl, 2:4] = high[at : at + 2]


def first_kernel(place, a0, a1, a3, a2, b0, b1, b3, b2, low, high, out, sems):
    _, y, zl, x = place[:4]
    copies = Copies(sems)
    row, col = lax.rem(y + 2, 4), lax.rem(x + 2, 4)
    other = 1 - zl
    for piece, by in ((a0, 0), (a1, 3), (a3, 1)):
        copies.start(piece, out.at[0, lax.rem(y + by, 4)], True)
    for piece, by in ((b0, 0), (b1, 3), (b3, 1)):
        for k in range(2):
            copies.start(piece.at[k], out.at[1, :, k, lax.rem(x + by, 4)], True)
    copies.start(a2, out.at[0, row, zl], True)
    copies.start(b2, out.at[1, :, zl, col], True)
    for k, part in enumerate((low, high)):
        copies.start(part.at[0:2], out.at[0, row, other, pl.ds(2 * k, 2)], True)
        copies.start(part.at[2:4], out.at[1, pl.ds(2 * k, 2), other, col], True)
    copies.finish()


def second_order_kernel(place, *refs):
    pieces, out, sems = refs[:8], refs[8], refs[9]
    core, y, x = place[0], place[1], place[3]
    copies = Copies(sems)
    for piece, by in zip(pieces[:4], (0, 3, 1, 2)):
        copies.start(piece, out.at[0, local_slot(lax.rem(y + by, 4), core)], True)
    for piece, by in zip(pieces[4:], (0, 3, 1, 2)):
        for k in range(2):
            copies.start(piece.at[k], out.at[1, :, k, lax.rem(x + by, 4)], True)
    copies.finish()


def hashed_signs(index, seed_term):
    h = index * 747796405 + seed_term
    h = h ^ lax.shift_right_logical(h, jnp.int32(15))
    h = h * 668265261
    h = h ^ lax.shift_right_logical(h, jnp.int32(13))
    h = h * 1274126177
    h = h ^ lax.shift_right_logical(h, jnp.int32(16))
    return jnp.where(h & 1 == 1, 1.0, -1.0).astype(bf16)


def local_quarter(core, j):
    return lax.rem(core + lax.div(j, 2), 2) + 2 * lax.rem(j, 2)


def signs_kernel(half, seed, out):
    core, j = lax.axis_index("core"), pl.program_id(0)
    rows = local_quarter(core, 2 * half + lax.div(j, 4)) * 512
    cols = local_quarter(core, lax.rem(j, 4)) * 512
    seed_term = seed[0] * 1664525 + 374761393
    r = lax.broadcasted_iota(jnp.int32, (512, 512), 0) + rows
    s = lax.broadcasted_iota(jnp.int32, (512, 512), 1) + cols
    out[...] = hashed_signs(r * 2048 + s, seed_term)


def sign_table(seed, half):
    return pl.pallas_call(
        functools.partial(signs_kernel, half),
        grid=(8,),
        in_specs=[pl.BlockSpec(memory_space=pltpu.SMEM)],
        out_specs=pl.BlockSpec((512, 512), lambda j: (j // 4, j % 4)),
        out_shape=jax.ShapeDtypeStruct((1024, 2048), bf16),
        compiler_params=pltpu.CompilerParams(vmem_limit_bytes=8 * 1024 * 1024),
        cost_estimate=pl.CostEstimate(flops=1 << 32, bytes_accessed=1 << 22, transcendentals=0),
    )(seed)


def prepare_kernel(place, hidden, gain, normed, tangent):
    values = hidden[...].astype(f32)
    inverse = lax.rsqrt(jnp.mean(values * values, axis=1, keepdims=True) + norm_eps)
    normed[...] = (values * inverse * gain[...].astype(f32)).astype(bf16)
    column = lax.broadcasted_iota(jnp.int32, (256, 512), 1)
    column = local_quarter(place[0], lax.div(column, 128)) * 128 + lax.rem(column, 128)
    total = jnp.zeros((512, 512), f32)
    for k in range(8):
        r = lax.broadcasted_iota(jnp.int32, (256, 512), 0) + 256 * k
        signs = hashed_signs(r * 512 + column, place[5] * 1664525)
        total += dot(normed[:, 256 * k : 256 * k + 256], signs)
    tangent[...] = (total * 2048 ** (-0.5)).astype(bf16)


def attention_kernel(half, place, n, w, tv, cos, sin, ctx_v, tctx_v, low_v, high_v, qkv):
    turn = lambda v, at: v * cos[at] + pltpu.roll(v, 64, 1) * sin[at]
    row = lax.rem(lax.broadcasted_iota(jnp.int32, (512, 128), 0), 128)
    over = row >= lax.broadcasted_iota(jnp.int32, (512, 128), 1)
    for k in range(2):
        qkv[k] = dot(n[...], w[k])

    def weights_of(parts):
        most = functools.reduce(jnp.maximum, parts)
        most = jnp.max(most, 1, keepdims=True)
        raised = [jnp.exp((v - most) * HEAD_DIM ** (-0.5)) for v in parts]
        share = 1.0 / jnp.sum(functools.reduce(jnp.add, raised), 1, keepdims=True)
        return [(v * share).astype(bf16) for v in raised]

    for k in range(2):
        for s in range(2):
            at = (slice(SEQ * s, SEQ * s + 128), slice(SEQ * s + 128, SEQ * s + SEQ))
            turns = (slice(0, 128), slice(128, 256))
            keys = [turn(qkv[k, r, 512:640], t).astype(bf16) for r, t in zip(at, turns)]
            query = [
                jnp.concatenate([turn(qkv[k, r, 128 * h : 128 * h + 128], t).astype(bf16) for h in range(4)], 0)
                for r, t in zip(at, turns)
            ]
            mix_at = slice(256 * half + 128 * k, 256 * half + 128 * k + 128)
            both = [jnp.concatenate([qkv[k, r, 640:768].astype(bf16), tv[r, mix_at]], 1) for r in at]
            score = lambda q, key: lax.dot_general(q, key, LAST, preferred_element_type=f32)
            masked = lambda v: jnp.where(over, v, -1e30)
            (low,) = weights_of([masked(score(query[0], keys[0]))])
            high = weights_of([score(query[1], keys[0]), masked(score(query[1], keys[1]))])
            low_v[s, k] = low
            high_v[s, k, :, 0:128] = high[0]
            high_v[s, k, :, 128:256] = high[1]
            mixed = (dot(low, both[0]).astype(bf16), (dot(high[0], both[0]) + dot(high[1], both[1])).astype(bf16))
            for value, r in zip(mixed, at):
                for h in range(4):
                    to = slice(512 * k + 128 * h, 512 * k + 128 * h + 128)
                    ctx_v[r, to] = value[128 * h : 128 * h + 128, :128]
                    tctx_v[r, to] = value[128 * h : 128 * h + 128, 128:]


def probe_kernel(place, ctx, signs, *refs):
    out = refs[-1]
    for j in range(4):
        cols = slice(512 * j, 512 * j + 512)
        value = dot(ctx[...], signs[:, cols]) * 2048 ** (-0.5)
        if len(refs) > 1:
            value += refs[0][:, cols].astype(f32)
        out[:, cols] = value.astype(bf16)


def cotangent_kernel(at, place, c0, c1, t0, t1, w, part, *refs):
    back_in, (term, back, cot) = refs[:-3], refs[-3:]
    for k in range(2):
        value = dot(t0[...], w[k, 0:1024]) + dot(t1[...], w[k, 1024:2048])
        here = slice(at + 512 * k, at + 512 * k + 512)
        cot[:, 512 * k : 512 * k + 512] = (value + part[:, here].astype(f32)).astype(bf16)
    for j, c in enumerate((c0, c1)):
        term[1024 * j : 1024 * j + 1024] = lax.dot_general(
            c[...], cot[...], ROWS, preferred_element_type=f32
        ).astype(bf16)
    for j in range(2):
        rows = slice(1024 * j, 1024 * j + 1024)
        value = lax.dot_general(cot[:, 0:512], w[0, rows], LAST, preferred_element_type=f32) + lax.dot_general(
            cot[:, 512:1024], w[1, rows], LAST, preferred_element_type=f32
        )
        if back_in:
            value += back_in[0][:, 1024 * (1 - j) : 1024 * (1 - j) + 1024].astype(f32)
        back[:, rows] = value.astype(bf16)


def value_kernel(place, n, lo0, lo1, hi0, hi1, back, own, partner, bv):
    spread = lambda p, up: lax.dot_general(p, up, ROWS, preferred_element_type=f32)
    for half, (lo, hi) in enumerate(((lo0, hi0), (lo1, hi1))):
        for k in range(2):
            at = 2 * half + k
            to = slice(128 * at, 128 * at + 128)
            for s in range(2):
                rows = (slice(SEQ * s, SEQ * s + 128), slice(SEQ * s + 128, SEQ * s + SEQ))
                head = lambda r, h: back[r, 512 * at + 128 * h : 512 * at + 128 * h + 128]
                up = [jnp.concatenate([head(r, h) for h in range(4)], 0) for r in rows]
                both = spread(hi[s, k], up[1])
                bv[rows[0], to] = (both[0:128] + spread(lo[s, k], up[0])).astype(bf16)
                bv[rows[1], to] = both[128:256].astype(bf16)
    for out, cols in ((partner, slice(256, 512)), (own, slice(0, 256))):
        out[...] = lax.dot_general(n[...], bv[:, cols], ROWS, preferred_element_type=f32).astype(bf16)


def pair_kernel(local, place, own, got, *refs):
    a, b = refs[:4], refs[4:8]
    core, y, x = place[0], place[1], place[3]
    add = lambda u, v: (u.astype(f32) + v.astype(f32)).astype(bf16)
    for by in range(4):
        row = lax.rem(y + by, 4)
        at = local_slot(row, core) if local else row
        for to in range(4):
            slot = lax.rem(x + to, 4)
            a[to][row] = add(own[at, :, slot, 0:32], got[at, :, slot, 0:32])
        b[by][...] = add(own[at, :, :, 32:64], got[at, :, :, 32:64])


def total_of(refs, index=()):
    total = refs[0][index].astype(f32)
    for r in refs[1:]:
        total += r[index].astype(f32)
    return total


def second_kernel(place, *refs):
    y, x = place[1], place[3]
    out_a, out_b = refs[16:20], refs[20:24]
    for cols, a, b in ((slice(0, 1024), refs[0:4], refs[4:8]), (slice(1024, 1280), refs[8:12], refs[12:16])):
        for by in range(4):
            out_a[by][:, :, cols] = total_of(a, lax.rem(y + by, 4)).astype(bf16)
            slot = lax.rem(x + by, 4)
            for zl in range(2):
                out_b[by][zl, :, cols] = total_of(b, (zl, slot)).astype(bf16)


def third_kernel(place, *refs):
    z = 2 * place[4] + place[2]
    a, b, out = refs[:4], refs[4:8], refs[8:]
    for by in range(4):
        to = lax.rem(z + by, 4)
        zl, zh = lax.rem(to, 2), lax.div(to, 2)
        for rows, parts in ((slice(0, 32), a), (slice(32, 64), b)):
            lo = total_of(parts, zl)
            for at, width in ((0, 512), (1024, 128)):
                left, right = lo[:, at : at + width], lo[:, at + width : at + 2 * width]
                got = jnp.where(zh == 0, left, right).astype(bf16)
                start = 0 if at == 0 else 512
                out[by][rows, start : start + width] = got


def last_kernel(place, own, before, after, across, value, output):
    total = total_of((own, before, after, across), slice(None))
    output[...] = total[:, :512]
    value[...] = total[:, 512:]


def exchanged(pieces, axis):
    return (pieces[0],) + tuple(shifted(pieces[by], axis, by) for by in (1, 3, 2))


def turn_tables():
    position = lax.broadcasted_iota(jnp.int32, (SEQ, 1), 0).astype(f32)
    exponent = lax.broadcasted_iota(jnp.int32, (1, 64), 1).astype(f32) * (-2.0 / HEAD_DIM)
    angles = position * jnp.power(f32(rope_base), exponent)
    cos, sin = jnp.cos(angles), jnp.sin(angles)
    return jnp.concatenate([cos, cos], 1), jnp.concatenate([-sin, sin], 1)


def step(hidden, norm_gain, query_weight, key_weight, value_weight, output_weight, probe_seed):
    vmem = lambda *shape: pltpu.VMEM(shape, bf16)

    a, b = call(
        cut_kernel, (query_weight, key_weight, value_weight, output_weight), [(64, 1280)] * 2,
        [dma(8)], kept=range(4), limit=60,
    )
    aq, ao, bq, bo, low_q, high_q, low_o, high_o = call(
        small_kernel, line_of(a, "x") + line_of(b, "y"),
        [(4, 64, 768), (4, 64, 512)] * 2 + [(4, 64, 768)] * 2 + [(4, 64, 512)] * 2, limit=10,
    )

    def joined(one, two, low, high):
        parts = (shifted(low, Z, -1), shifted(high, Z, 1))
        return call(join_kernel, (one, two, *parts), [(2,) + one.shape] * 2, limit=8)

    a_first, b_first = joined(aq, bq, low_q, high_q)
    a_across, b_across = shifted(aq, "y", 2), shifted(bq, "x", 2)
    a_lines = [shifted(a_first, "y", by) for by in (1, -1)]
    b_lines = [shifted(b_first, "x", by) for by in (1, -1)]
    part_of = lambda k: jnp.concatenate([v[2 * k : 2 * k + 2] for v in (a_across, b_across)], 0)
    z_low, z_high = shifted(part_of(0), Z, -1), shifted(part_of(1), Z, 1)
    (w_own,) = call(
        first_kernel,
        (a_first, *a_lines, a_across, b_first, *b_lines, b_across, z_low, z_high),
        [(2, 4, 2, 4, 64, 768)], [dma(15)], far=(0,), limit=8,
    )
    w_own = w_own.reshape(2, 2048, 768)
    w_partner = shifted(w_own, "core", 1)
    a_second, b_second = joined(ao, bo, low_o, high_o)
    (o_own,) = call(
        second_order_kernel, line_of(a_second, "y") + line_of(b_second, "x"),
        [(2, 4, 2, 4, 64, 512)], [dma(12)], far=(0,), limit=8,
    )
    o_own = o_own.reshape(2, 2048, 512)
    o_partner = shifted(o_own, "core", 1)

    hidden, cos, sin = lax.optimization_barrier((hidden, *turn_tables()))
    normed, tangent_value = call(
        prepare_kernel, (hidden, norm_gain.reshape(1, 2048)), [(512, 2048), (512, 512)],
        flops=2 << 30, limit=20, seed=probe_seed,
    )
    signs0, signs1 = sign_table(probe_seed, 0), sign_table(probe_seed, 1)

    def attend(w, half):
        return call(
            functools.partial(attention_kernel, half), (normed, w, tangent_value, cos, sin),
            [(512, 1024), (512, 1024), (2, 2, 512, 128), (2, 2, 512, 256)],
            [pltpu.VMEM((2, 512, 768), f32)], flops=5 << 30, limit=LIMITS[0],
        )

    c_own, t_own, low_own, high_own = attend(w_own, 0)
    c_partner, t_partner, low_partner, high_partner = attend(w_partner, 1)
    probe = lambda *args: call(probe_kernel, args, [(512, 2048)], flops=2 << 30, limit=LIMITS[1])[0]
    part = probe(c_partner, signs1, probe(c_own, signs0))

    def cotangent(at, *args):
        return call(
            functools.partial(cotangent_kernel, at), args, [(2048, 1024), (512, 2048)],
            [vmem(512, 1024)], flops=6 << 30, limit=LIMITS[2],
        )

    term_partner, back = cotangent(1024, c_partner, c_own, t_partner, t_own, o_partner, part)
    term_own, back = cotangent(0, c_own, c_partner, t_own, t_partner, o_own, part, back)
    grid = lambda v: v.reshape(4, 2, 4, 64, v.shape[1])

    def paired(local, own, partner):
        got = shifted(partner, "core", 1)
        n = own.shape[1]
        pieces = call(
            functools.partial(pair_kernel, local), (grid(own), grid(got)),
            [(4, 2, 32, n)] * 4 + [(2, 4, 32, n)] * 4,
            limit=LIMITS[4],
        )
        return exchanged(pieces[:4], "x") + exchanged(pieces[4:], "y")

    out_pieces = paired(True, term_own, term_partner)
    val_own, val_partner = call(
        value_kernel,
        (normed, low_own, low_partner, high_own, high_partner, back), [(2048, 256)] * 2,
        [vmem(512, 512)], flops=2 << 30, limit=LIMITS[3],
    )
    val_pieces = paired(False, val_own, val_partner)
    pieces = call(second_kernel, out_pieces + val_pieces, [(2, 32, 1280)] * 8, limit=20)
    pieces = call(
        third_kernel, exchanged(pieces[:4], "y") + exchanged(pieces[4:], "x"),
        [(64, 640)] * 4, limit=8,
    )
    value, output = call(last_kernel, exchanged(pieces, Z), [(64, 128), (64, 512)], dtypes=[f32, f32], limit=4)
    return value, output


def solution(mesh):
    fine = Mesh(mesh.devices.reshape(2, 2, 4, 2, 4), AXES)
    fsdp, probe = ("y", "zl", "x"), ("zh", "core")
    return jax.shard_map(
        step,
        mesh=fine,
        in_specs=(P(AXES, None), P(), P(fsdp, None), P(fsdp, None), P(fsdp, None), P(fsdp, None), P(probe)),
        out_specs=(P(fsdp, probe), P(fsdp, probe)),
        check_vma=False,
    )
```

```python
import functools

import jax
import jax.numpy as jnp
from jax import lax
from jax.experimental import pallas as pl
from jax.experimental.pallas import tpu as pltpu
from jax.sharding import Mesh
from jax.sharding import PartitionSpec as P

HEAD_DIM = 128
SEQ = 256
AXES = ("zh", "core", "y", "zl", "x")
Z = ("zh", "zl")
norm_eps = 1e-05
rope_base = 500000.0
LIMITS = (14, 8, 12, 10, 6)
bf16, f32 = jnp.bfloat16, jnp.float32
ROWS = (((0,), (0,)), ((), ()))
LAST = (((1,), (1,)), ((), ()))


def dot(a, b):
    return jnp.dot(a, b, preferred_element_type=f32)


def position(seed=None):
    core, y, zl, x, zh = (lax.axis_index(a) for a in ("core", "y", "zl", "x", "zh"))
    return core, y, zl, x, zh, None if seed is None else seed[0]


def call(kernel, args, shapes, scratch=(), flops=0, kept=(), far=(), dtypes=None, limit=56, seed=None):
    dtypes = dtypes or [bf16] * len(shapes)
    space = lambda i, there: pl.BlockSpec(memory_space=pltpu.HBM if i in there else pltpu.VMEM)
    moved = sum(a.size * a.dtype.itemsize for a in args)
    in_specs = [space(i, kept) for i in range(len(args))]
    if seed is None:
        run = lambda *refs: kernel(position(), *refs)
    else:
        in_specs, args = [pl.BlockSpec(memory_space=pltpu.SMEM)] + in_specs, (seed,) + tuple(args)
        run = lambda ref, *refs: kernel(position(ref), *refs)
    return pl.pallas_call(
        run,
        in_specs=in_specs,
        out_specs=[space(i, far) for i in range(len(shapes))],
        out_shape=[jax.ShapeDtypeStruct(s, d) for s, d in zip(shapes, dtypes)],
        scratch_shapes=list(scratch),
        compiler_params=pltpu.CompilerParams(vmem_limit_bytes=limit * 1024 * 1024),
        cost_estimate=pl.CostEstimate(flops=flops or moved // 2, bytes_accessed=moved, transcendentals=0),
    )(*args)


class Copies:
    def __init__(self, sems):
        self.sems, self.used, self.open = sems, 0, []

    def start(self, source, target, late=False):
        copy = pltpu.make_async_copy(source, target, self.sems.at[self.used])
        self.used += 1
        copy.start()
        if late:
            self.open.append(copy)
        return copy

    def finish(self):
        for copy in self.open:
            copy.wait()


def dma(count):
    return pltpu.SemaphoreType.DMA((count,))


def shifted(value, axis, by):
    size = lax.axis_size(axis)
    return lax.ppermute(value, axis, [(i, (i + by) % size) for i in range(size)])


def line_of(value, axis):
    return (value,) + tuple(shifted(value, axis, by) for by in (1, -1, 2))


def local_slot(y, core):
    return lax.div(y, 2) + 2 * lax.rem(lax.rem(y, 2) + core, 2)


def cut_kernel(place, q, k, v, o, a, b, sems):
    copies = Copies(sems)
    for color, out in enumerate((a, b)):
        p = 2 * color + place[0]
        for ref, width, to in ((q, 512, 0), (k, 128, 512), (v, 128, 640), (o, 512, 768)):
            cols = pl.ds(pl.multiple_of(p * width, width), width)
            copies.start(ref.at[:, cols], out.at[:, pl.ds(to, width)], True)
    copies.finish()


def small_kernel(place, *refs):
    aq, ao, bq, bo, low_q, high_q, low_o, high_o = refs[8:]
    core, y, _, x = place[:4]
    for k, by in enumerate((0, 3, 1, 2)):
        slot = lax.rem(x + by, 4)
        aq[slot] = refs[k][:, :768]
        ao[slot] = refs[k][:, 768:]
        slot = lax.rem(y + by, 4)
        bq[slot] = refs[4 + k][:, :768]
        bo[local_slot(slot, core)] = refs[4 + k][:, 768:]
    for low, high, a, b in ((low_q, high_q, aq, bq), (low_o, high_o, ao, bo)):
        for out, half in ((low, slice(0, 2)), (high, slice(2, 4))):
            out[0:2] = a[half]
            out[2:4] = b[half]


def join_kernel(place, a, b, low, high, out_a, out_b):
    zl = place[2]
    for own, out, at in ((a, out_a, 0), (b, out_b, 2)):
        out[zl] = own[...]
        out[1 - zl, 0:2] = low[at : at + 2]
        out[1 - zl, 2:4] = high[at : at + 2]


def split_kernel(place, a, b, low, high):
    for out, half in ((low, slice(0, 2)), (high, slice(2, 4))):
        out[0:2] = a[half]
        out[2:4] = b[half]


def order_kernel(local, place, a0, a1, a3, a2, b0, b1, b3, b2, low, high, out, sems):
    core, y, zl, x = place[:4]
    copies = Copies(sems)
    row = (lambda by: local_slot(lax.rem(y + by, 4), core)) if local else (lambda by: lax.rem(y + by, 4))
    col = lambda by: lax.rem(x + by, 4)
    other = 1 - zl
    for piece, by in ((a0, 0), (a1, 3), (a3, 1)):
        copies.start(piece, out.at[0, row(by)], True)
    for piece, by in ((b0, 0), (b1, 3), (b3, 1)):
        for k in range(2):
            copies.start(piece.at[k], out.at[1, :, k, col(by)], True)
    copies.start(a2, out.at[0, row(2), zl], True)
    copies.start(b2, out.at[1, :, zl, col(2)], True)
    for k, part in enumerate((low, high)):
        copies.start(part.at[0:2], out.at[0, row(2), other, pl.ds(2 * k, 2)], True)
        copies.start(part.at[2:4], out.at[1, pl.ds(2 * k, 2), other, col(2)], True)
    copies.finish()


def hashed_signs(index, seed_term):
    h = index * 747796405 + seed_term
    h = h ^ lax.shift_right_logical(h, jnp.int32(15))
    h = h * 668265261
    h = h ^ lax.shift_right_logical(h, jnp.int32(13))
    h = h * 1274126177
    h = h ^ lax.shift_right_logical(h, jnp.int32(16))
    return jnp.where(h & 1 == 1, 1.0, -1.0).astype(bf16)


def local_quarter(core, j):
    return lax.rem(core + lax.div(j, 2), 2) + 2 * lax.rem(j, 2)


def signs_kernel(half, seed, out):
    core, j = lax.axis_index("core"), pl.program_id(0)
    rows = local_quarter(core, 2 * half + lax.div(j, 4)) * 512
    cols = local_quarter(core, lax.rem(j, 4)) * 512
    seed_term = seed[0] * 1664525 + 374761393
    r = lax.broadcasted_iota(jnp.int32, (512, 512), 0) + rows
    s = lax.broadcasted_iota(jnp.int32, (512, 512), 1) + cols
    out[...] = hashed_signs(r * 2048 + s, seed_term)


def sign_table(seed, half):
    return pl.pallas_call(
        functools.partial(signs_kernel, half),
        grid=(8,),
        in_specs=[pl.BlockSpec(memory_space=pltpu.SMEM)],
        out_specs=pl.BlockSpec((512, 512), lambda j: (j // 4, j % 4)),
        out_shape=jax.ShapeDtypeStruct((1024, 2048), bf16),
        compiler_params=pltpu.CompilerParams(vmem_limit_bytes=8 * 1024 * 1024),
        cost_estimate=pl.CostEstimate(flops=1 << 32, bytes_accessed=1 << 22, transcendentals=0),
    )(seed)


def prepare_kernel(place, hidden, gain, normed, tangent):
    values = hidden[...].astype(f32)
    inverse = lax.rsqrt(jnp.mean(values * values, axis=1, keepdims=True) + norm_eps)
    normed[...] = (values * inverse * gain[...].astype(f32)).astype(bf16)
    column = lax.broadcasted_iota(jnp.int32, (256, 512), 1)
    column = local_quarter(place[0], lax.div(column, 128)) * 128 + lax.rem(column, 128)
    total = jnp.zeros((512, 512), f32)
    for k in range(8):
        r = lax.broadcasted_iota(jnp.int32, (256, 512), 0) + 256 * k
        signs = hashed_signs(r * 512 + column, place[5] * 1664525)
        total += dot(normed[:, 256 * k : 256 * k + 256], signs)
    tangent[...] = (total * 2048 ** (-0.5)).astype(bf16)


def attention_kernel(half, place, n, w, tv, cos, sin, ctx_v, tctx_v, low_v, high_v, qkv):
    turn = lambda v, at: v * cos[at] + pltpu.roll(v, 64, 1) * sin[at]
    row = lax.rem(lax.broadcasted_iota(jnp.int32, (512, 128), 0), 128)
    over = row >= lax.broadcasted_iota(jnp.int32, (512, 128), 1)
    for k in range(2):
        qkv[k] = dot(n[...], w[k])

    def weights_of(parts):
        most = functools.reduce(jnp.maximum, parts)
        most = jnp.max(most, 1, keepdims=True)
        raised = [jnp.exp((v - most) * HEAD_DIM ** (-0.5)) for v in parts]
        share = 1.0 / jnp.sum(functools.reduce(jnp.add, raised), 1, keepdims=True)
        return [(v * share).astype(bf16) for v in raised]

    for k in range(2):
        for s in range(2):
            at = (slice(SEQ * s, SEQ * s + 128), slice(SEQ * s + 128, SEQ * s + SEQ))
            turns = (slice(0, 128), slice(128, 256))
            keys = [turn(qkv[k, r, 512:640], t).astype(bf16) for r, t in zip(at, turns)]
            query = [
                jnp.concatenate([turn(qkv[k, r, 128 * h : 128 * h + 128], t).astype(bf16) for h in range(4)], 0)
                for r, t in zip(at, turns)
            ]
            mix_at = slice(256 * half + 128 * k, 256 * half + 128 * k + 128)
            both = [jnp.concatenate([qkv[k, r, 640:768].astype(bf16), tv[r, mix_at]], 1) for r in at]
            score = lambda q, key: lax.dot_general(q, key, LAST, preferred_element_type=f32)
            masked = lambda v: jnp.where(over, v, -1e30)
            (low,) = weights_of([masked(score(query[0], keys[0]))])
            high = weights_of([score(query[1], keys[0]), masked(score(query[1], keys[1]))])
            low_v[s, k] = low
            high_v[s, k, :, 0:128] = high[0]
            high_v[s, k, :, 128:256] = high[1]
            mixed = (dot(low, both[0]).astype(bf16), (dot(high[0], both[0]) + dot(high[1], both[1])).astype(bf16))
            for value, r in zip(mixed, at):
                for h in range(4):
                    to = slice(512 * k + 128 * h, 512 * k + 128 * h + 128)
                    ctx_v[r, to] = value[128 * h : 128 * h + 128, :128]
                    tctx_v[r, to] = value[128 * h : 128 * h + 128, 128:]


def probe_kernel(place, ctx, signs, *refs):
    out = refs[-1]
    for j in range(4):
        cols = slice(512 * j, 512 * j + 512)
        value = dot(ctx[...], signs[:, cols]) * 2048 ** (-0.5)
        if len(refs) > 1:
            value += refs[0][:, cols].astype(f32)
        out[:, cols] = value.astype(bf16)


def cotangent_kernel(at, place, c0, c1, t0, t1, w, part, *refs):
    back_in, (term, back, cot) = refs[:-3], refs[-3:]
    for k in range(2):
        value = dot(t0[...], w[k, 0:1024]) + dot(t1[...], w[k, 1024:2048])
        here = slice(at + 512 * k, at + 512 * k + 512)
        cot[:, 512 * k : 512 * k + 512] = (value + part[:, here].astype(f32)).astype(bf16)
    for j, c in enumerate((c0, c1)):
        term[1024 * j : 1024 * j + 1024] = lax.dot_general(
            c[...], cot[...], ROWS, preferred_element_type=f32
        ).astype(bf16)
    for j in range(2):
        rows = slice(1024 * j, 1024 * j + 1024)
        value = lax.dot_general(cot[:, 0:512], w[0, rows], LAST, preferred_element_type=f32) + lax.dot_general(
            cot[:, 512:1024], w[1, rows], LAST, preferred_element_type=f32
        )
        if back_in:
            value += back_in[0][:, 1024 * (1 - j) : 1024 * (1 - j) + 1024].astype(f32)
        back[:, rows] = value.astype(bf16)


def value_kernel(place, n, lo0, lo1, hi0, hi1, back, own, partner, bv):
    spread = lambda p, up: lax.dot_general(p, up, ROWS, preferred_element_type=f32)
    for half, (lo, hi) in enumerate(((lo0, hi0), (lo1, hi1))):
        for k in range(2):
            at = 2 * half + k
            to = slice(128 * at, 128 * at + 128)
            for s in range(2):
                rows = (slice(SEQ * s, SEQ * s + 128), slice(SEQ * s + 128, SEQ * s + SEQ))
                head = lambda r, h: back[r, 512 * at + 128 * h : 512 * at + 128 * h + 128]
                up = [jnp.concatenate([head(r, h) for h in range(4)], 0) for r in rows]
                both = spread(hi[s, k], up[1])
                bv[rows[0], to] = (both[0:128] + spread(lo[s, k], up[0])).astype(bf16)
                bv[rows[1], to] = both[128:256].astype(bf16)
    for out, cols in ((partner, slice(256, 512)), (own, slice(0, 256))):
        out[...] = lax.dot_general(n[...], bv[:, cols], ROWS, preferred_element_type=f32).astype(bf16)


def pair_kernel(local, place, own, got, *refs):
    a, b = refs[:4], refs[4:8]
    core, y, x = place[0], place[1], place[3]
    add = lambda u, v: (u.astype(f32) + v.astype(f32)).astype(bf16)
    for by in range(4):
        row = lax.rem(y + by, 4)
        at = local_slot(row, core) if local else row
        for to in range(4):
            slot = lax.rem(x + to, 4)
            a[to][row] = add(own[at, :, slot, 0:32], got[at, :, slot, 0:32])
        b[by][...] = add(own[at, :, :, 32:64], got[at, :, :, 32:64])


def total_of(refs, index=()):
    total = refs[0][index].astype(f32)
    for r in refs[1:]:
        total += r[index].astype(f32)
    return total


def second_kernel(place, *refs):
    y, x = place[1], place[3]
    out_a, out_b = refs[16:20], refs[20:24]
    for cols, a, b in ((slice(0, 1024), refs[0:4], refs[4:8]), (slice(1024, 1280), refs[8:12], refs[12:16])):
        for by in range(4):
            out_a[by][:, :, cols] = total_of(a, lax.rem(y + by, 4)).astype(bf16)
            slot = lax.rem(x + by, 4)
            for zl in range(2):
                out_b[by][zl, :, cols] = total_of(b, (zl, slot)).astype(bf16)


def third_kernel(place, *refs):
    z = 2 * place[4] + place[2]
    a, b, out = refs[:4], refs[4:8], refs[8:]
    for by in range(4):
        to = lax.rem(z + by, 4)
        zl, zh = lax.rem(to, 2), lax.div(to, 2)
        for rows, parts in ((slice(0, 32), a), (slice(32, 64), b)):
            lo = total_of(parts, zl)
            for at, width in ((0, 512), (1024, 128)):
                left, right = lo[:, at : at + width], lo[:, at + width : at + 2 * width]
                got = jnp.where(zh == 0, left, right).astype(bf16)
                start = 0 if at == 0 else 512
                out[by][rows, start : start + width] = got


def last_kernel(place, own, before, after, across, value, output):
    total = total_of((own, before, after, across), slice(None))
    output[...] = total[:, :512]
    value[...] = total[:, 512:]


def exchanged(pieces, axis):
    return (pieces[0],) + tuple(shifted(pieces[by], axis, by) for by in (1, 3, 2))


def turn_tables():
    position = lax.broadcasted_iota(jnp.int32, (SEQ, 1), 0).astype(f32)
    exponent = lax.broadcasted_iota(jnp.int32, (1, 64), 1).astype(f32) * (-2.0 / HEAD_DIM)
    angles = position * jnp.power(f32(rope_base), exponent)
    cos, sin = jnp.cos(angles), jnp.sin(angles)
    return jnp.concatenate([cos, cos], 1), jnp.concatenate([-sin, sin], 1)


def step(hidden, norm_gain, query_weight, key_weight, value_weight, output_weight, probe_seed):
    vmem = lambda *shape: pltpu.VMEM(shape, bf16)

    a, b = call(
        cut_kernel, (query_weight, key_weight, value_weight, output_weight), [(64, 1280)] * 2,
        [dma(8)], kept=range(4), limit=60,
    )
    aq, ao, bq, bo, low_q, high_q, low_o, high_o = call(
        small_kernel, line_of(a, "x") + line_of(b, "y"),
        [(4, 64, 768), (4, 64, 512)] * 2 + [(4, 64, 768)] * 2 + [(4, 64, 512)] * 2, limit=10,
    )

    def gathered(local, a, b, low, high):
        n = a.shape[2]
        z_pair = lambda parts: (shifted(parts[0], Z, -1), shifted(parts[1], Z, 1))
        across = shifted(a, "y", 2), shifted(b, "x", 2)
        fa, fb = call(join_kernel, (a, b, *z_pair((low, high))), [(2, 4, 64, n)] * 2, limit=8)
        la = [shifted(fa, "y", by) for by in (1, -1)]
        lb = [shifted(fb, "x", by) for by in (1, -1)]
        rest = z_pair(call(split_kernel, across, [(4, 64, n)] * 2, limit=8))
        (w,) = call(
            functools.partial(order_kernel, local),
            (fa, *la, across[0], fb, *lb, across[1], *rest),
            [(2, 4, 2, 4, 64, n)], [dma(15)], far=(0,), limit=8,
        )
        return w.reshape(2, 2048, n)

    w_own = gathered(False, aq, bq, low_q, high_q)
    w_partner = shifted(w_own, "core", 1)
    o_own = gathered(True, ao, bo, low_o, high_o)
    o_partner = shifted(o_own, "core", 1)

    hidden, cos, sin = lax.optimization_barrier((hidden, *turn_tables()))
    normed, tangent_value = call(
        prepare_kernel, (hidden, norm_gain.reshape(1, 2048)), [(512, 2048), (512, 512)],
        flops=2 << 30, limit=20, seed=probe_seed,
    )
    signs0, signs1 = sign_table(probe_seed, 0), sign_table(probe_seed, 1)

    def attend(w, half):
        return call(
            functools.partial(attention_kernel, half), (normed, w, tangent_value, cos, sin),
            [(512, 1024), (512, 1024), (2, 2, 512, 128), (2, 2, 512, 256)],
            [pltpu.VMEM((2, 512, 768), f32)], flops=5 << 30, limit=LIMITS[0],
        )

    c_own, t_own, low_own, high_own = attend(w_own, 0)
    c_partner, t_partner, low_partner, high_partner = attend(w_partner, 1)
    probe = lambda *args: call(probe_kernel, args, [(512, 2048)], flops=2 << 30, limit=LIMITS[1])[0]
    part = probe(c_partner, signs1, probe(c_own, signs0))

    def cotangent(at, *args):
        return call(
            functools.partial(cotangent_kernel, at), args, [(2048, 1024), (512, 2048)],
            [vmem(512, 1024)], flops=6 << 30, limit=LIMITS[2],
        )

    term_partner, back = cotangent(1024, c_partner, c_own, t_partner, t_own, o_partner, part)
    term_own, back = cotangent(0, c_own, c_partner, t_own, t_partner, o_own, part, back)
    grid = lambda v: v.reshape(4, 2, 4, 64, v.shape[1])

    def paired(local, own, partner):
        got = shifted(partner, "core", 1)
        n = own.shape[1]
        pieces = call(
            functools.partial(pair_kernel, local), (grid(own), grid(got)),
            [(4, 2, 32, n)] * 4 + [(2, 4, 32, n)] * 4,
            limit=LIMITS[4],
        )
        return exchanged(pieces[:4], "x") + exchanged(pieces[4:], "y")

    out_pieces = paired(True, term_own, term_partner)
    val_own, val_partner = call(
        value_kernel,
        (normed, low_own, low_partner, high_own, high_partner, back), [(2048, 256)] * 2,
        [vmem(512, 512)], flops=2 << 30, limit=LIMITS[3],
    )
    val_pieces = paired(False, val_own, val_partner)
    pieces = call(second_kernel, out_pieces + val_pieces, [(2, 32, 1280)] * 8, limit=20)
    pieces = call(
        third_kernel, exchanged(pieces[:4], "y") + exchanged(pieces[4:], "x"),
        [(64, 640)] * 4, limit=8,
    )
    value, output = call(last_kernel, exchanged(pieces, Z), [(64, 128), (64, 512)], dtypes=[f32, f32], limit=4)
    return value, output


def solution(mesh):
    fine = Mesh(mesh.devices.reshape(2, 2, 4, 2, 4), AXES)
    fsdp, probe = ("y", "zl", "x"), ("zh", "core")
    return jax.shard_map(
        step,
        mesh=fine,
        in_specs=(P(AXES, None), P(), P(fsdp, None), P(fsdp, None), P(fsdp, None), P(fsdp, None), P(probe)),
        out_specs=(P(fsdp, probe), P(fsdp, probe)),
        check_vma=False,
    )
```

```python
import functools

import jax
import jax.numpy as jnp
from jax import lax
from jax.experimental import pallas as pl
from jax.experimental.pallas import tpu as pltpu
from jax.sharding import Mesh
from jax.sharding import PartitionSpec as P

HEAD_DIM = 128
SEQ = 256
AXES = ("zh", "core", "y", "zl", "x")
Z = ("zh", "zl")
norm_eps = 1e-05
rope_base = 500000.0
LIMITS = (14, 8, 12, 10, 6)
bf16, f32 = jnp.bfloat16, jnp.float32
ROWS = (((0,), (0,)), ((), ()))
LAST = (((1,), (1,)), ((), ()))


def dot(a, b):
    return jnp.dot(a, b, preferred_element_type=f32)


def position(seed=None):
    core, y, zl, x, zh = (lax.axis_index(a) for a in ("core", "y", "zl", "x", "zh"))
    return core, y, zl, x, zh, None if seed is None else seed[0]


def call(kernel, args, shapes, scratch=(), flops=0, kept=(), far=(), dtypes=None, limit=56, seed=None):
    dtypes = dtypes or [bf16] * len(shapes)
    space = lambda i, there: pl.BlockSpec(memory_space=pltpu.HBM if i in there else pltpu.VMEM)
    moved = sum(a.size * a.dtype.itemsize for a in args)
    in_specs = [space(i, kept) for i in range(len(args))]
    if seed is None:
        run = lambda *refs: kernel(position(), *refs)
    else:
        in_specs, args = [pl.BlockSpec(memory_space=pltpu.SMEM)] + in_specs, (seed,) + tuple(args)
        run = lambda ref, *refs: kernel(position(ref), *refs)
    return pl.pallas_call(
        run,
        in_specs=in_specs,
        out_specs=[space(i, far) for i in range(len(shapes))],
        out_shape=[jax.ShapeDtypeStruct(s, d) for s, d in zip(shapes, dtypes)],
        scratch_shapes=list(scratch),
        compiler_params=pltpu.CompilerParams(vmem_limit_bytes=limit * 1024 * 1024),
        cost_estimate=pl.CostEstimate(flops=flops or moved // 2, bytes_accessed=moved, transcendentals=0),
    )(*args)


class Copies:
    def __init__(self, sems):
        self.sems, self.used, self.open = sems, 0, []

    def start(self, source, target, late=False):
        copy = pltpu.make_async_copy(source, target, self.sems.at[self.used])
        self.used += 1
        copy.start()
        if late:
            self.open.append(copy)
        return copy

    def finish(self):
        for copy in self.open:
            copy.wait()


def dma(count):
    return pltpu.SemaphoreType.DMA((count,))


def shifted(value, axis, by):
    size = lax.axis_size(axis)
    return lax.ppermute(value, axis, [(i, (i + by) % size) for i in range(size)])


def line_of(value, axis):
    return (value,) + tuple(shifted(value, axis, by) for by in (1, -1, 2))


def local_slot(y, core):
    return lax.div(y, 2) + 2 * lax.rem(lax.rem(y, 2) + core, 2)


def cut_kernel(place, q, k, v, o, a, b, sems):
    copies = Copies(sems)
    for color, out in enumerate((a, b)):
        p = 2 * color + place[0]
        for ref, width, to in ((q, 512, 0), (k, 128, 512), (v, 128, 640), (o, 512, 768)):
            cols = pl.ds(pl.multiple_of(p * width, width), width)
            copies.start(ref.at[:, cols], out.at[:, pl.ds(to, width)], True)
    copies.finish()


def small_kernel(place, *refs):
    aq, ao, bq, bo, low_q, high_q, low_o, high_o = refs[8:]
    core, y, _, x = place[:4]
    for k, by in enumerate((0, 3, 1, 2)):
        slot = lax.rem(x + by, 4)
        aq[slot] = refs[k][:, :768]
        ao[slot] = refs[k][:, 768:]
        slot = lax.rem(y + by, 4)
        bq[slot] = refs[4 + k][:, :768]
        bo[local_slot(slot, core)] = refs[4 + k][:, 768:]
    for low, high, a, b in ((low_q, high_q, aq, bq), (low_o, high_o, ao, bo)):
        for out, half in ((low, slice(0, 2)), (high, slice(2, 4))):
            out[0:2] = a[half]
            out[2:4] = b[half]


def join_kernel(place, a, b, low, high, out_a, out_b):
    zl = place[2]
    for own, out, at in ((a, out_a, 0), (b, out_b, 2)):
        out[zl] = own[...]
        out[1 - zl, 0:2] = low[at : at + 2]
        out[1 - zl, 2:4] = high[at : at + 2]


def split_kernel(place, a, b, low, high):
    for out, half in ((low, slice(0, 2)), (high, slice(2, 4))):
        out[0:2] = a[half]
        out[2:4] = b[half]


def order_kernel(local, place, a0, a1, a3, a2, b0, b1, b3, b2, low, high, out, sems):
    core, y, zl, x = place[:4]
    copies = Copies(sems)
    row = (lambda by: local_slot(lax.rem(y + by, 4), core)) if local else (lambda by: lax.rem(y + by, 4))
    col = lambda by: lax.rem(x + by, 4)
    other = 1 - zl
    for piece, by in ((a0, 0), (a1, 3), (a3, 1)):
        copies.start(piece, out.at[0, row(by)], True)
    for piece, by in ((b0, 0), (b1, 3), (b3, 1)):
        for k in range(2):
            copies.start(piece.at[k], out.at[1, :, k, col(by)], True)
    copies.start(a2, out.at[0, row(2), zl], True)
    copies.start(b2, out.at[1, :, zl, col(2)], True)
    for k, part in enumerate((low, high)):
        copies.start(part.at[0:2], out.at[0, row(2), other, pl.ds(2 * k, 2)], True)
        copies.start(part.at[2:4], out.at[1, pl.ds(2 * k, 2), other, col(2)], True)
    copies.finish()


def hashed_signs(row, column, width, seed_term):
    h = (row * ((width * 747796405 + (1 << 31)) % (1 << 32) - (1 << 31)) + seed_term) + column * 747796405
    h = h ^ lax.shift_right_logical(h, jnp.int32(15))
    h = h * 668265261
    h = h ^ lax.shift_right_logical(h, jnp.int32(13))
    h = h * 1274126177
    h = h ^ lax.shift_right_logical(h, jnp.int32(16))
    return jnp.where(h & 1 == 1, 1.0, -1.0).astype(bf16)


def local_quarter(core, j):
    return lax.rem(core + lax.div(j, 2), 2) + 2 * lax.rem(j, 2)


def signs_kernel(half, seed, out):
    core, j = lax.axis_index("core"), pl.program_id(0)
    rows = local_quarter(core, 2 * half + lax.div(j, 4)) * 512
    cols = local_quarter(core, lax.rem(j, 4)) * 512
    seed_term = seed[0] * 1664525 + 374761393
    r = lax.broadcasted_iota(jnp.int32, (512, 1), 0) + rows
    s = lax.broadcasted_iota(jnp.int32, (1, 512), 1) + cols
    out[...] = hashed_signs(r, s, 2048, seed_term)


def sign_table(seed, half):
    return pl.pallas_call(
        functools.partial(signs_kernel, half),
        grid=(8,),
        in_specs=[pl.BlockSpec(memory_space=pltpu.SMEM)],
        out_specs=pl.BlockSpec((512, 512), lambda j: (j // 4, j % 4)),
        out_shape=jax.ShapeDtypeStruct((1024, 2048), bf16),
        compiler_params=pltpu.CompilerParams(vmem_limit_bytes=8 * 1024 * 1024),
        cost_estimate=pl.CostEstimate(flops=1 << 32, bytes_accessed=1 << 22, transcendentals=0),
    )(seed)


def prepare_kernel(place, hidden, gain, normed, tangent):
    values = hidden[...].astype(f32)
    inverse = lax.rsqrt(jnp.mean(values * values, axis=1, keepdims=True) + norm_eps)
    normed[...] = (values * inverse * gain[...].astype(f32)).astype(bf16)
    column = lax.broadcasted_iota(jnp.int32, (1, 512), 1)
    column = local_quarter(place[0], lax.div(column, 128)) * 128 + lax.rem(column, 128)
    total = jnp.zeros((512, 512), f32)
    for k in range(8):
        r = lax.broadcasted_iota(jnp.int32, (256, 1), 0) + 256 * k
        signs = hashed_signs(r, column, 512, place[5] * 1664525)
        total += dot(normed[:, 256 * k : 256 * k + 256], signs)
    tangent[...] = (total * 2048 ** (-0.5)).astype(bf16)


def attention_kernel(half, place, n, w, tv, cos, sin, ctx_v, tctx_v, low_v, high_v, qkv):
    turn = lambda v, at: v * cos[at] + pltpu.roll(v, 64, 1) * sin[at]
    row = lax.rem(lax.broadcasted_iota(jnp.int32, (512, 128), 0), 128)
    over = row >= lax.broadcasted_iota(jnp.int32, (512, 128), 1)
    for k in range(2):
        qkv[k] = dot(n[...], w[k])

    def weights_of(parts):
        most = functools.reduce(jnp.maximum, parts)
        most = jnp.max(most, 1, keepdims=True)
        raised = [jnp.exp((v - most) * HEAD_DIM ** (-0.5)) for v in parts]
        share = 1.0 / jnp.sum(functools.reduce(jnp.add, raised), 1, keepdims=True)
        return [(v * share).astype(bf16) for v in raised]

    for k in range(2):
        for s in range(2):
            at = (slice(SEQ * s, SEQ * s + 128), slice(SEQ * s + 128, SEQ * s + SEQ))
            turns = (slice(0, 128), slice(128, 256))
            keys = [turn(qkv[k, r, 512:640], t).astype(bf16) for r, t in zip(at, turns)]
            query = [
                jnp.concatenate([turn(qkv[k, r, 128 * h : 128 * h + 128], t).astype(bf16) for h in range(4)], 0)
                for r, t in zip(at, turns)
            ]
            mix_at = slice(256 * half + 128 * k, 256 * half + 128 * k + 128)
            both = [jnp.concatenate([qkv[k, r, 640:768].astype(bf16), tv[r, mix_at]], 1) for r in at]
            score = lambda q, key: lax.dot_general(q, key, LAST, preferred_element_type=f32)
            masked = lambda v: jnp.where(over, v, -1e30)
            (low,) = weights_of([masked(score(query[0], keys[0]))])
            high = weights_of([score(query[1], keys[0]), masked(score(query[1], keys[1]))])
            low_v[s, k] = low
            high_v[s, k, :, 0:128] = high[0]
            high_v[s, k, :, 128:256] = high[1]
            mixed = (dot(low, both[0]).astype(bf16), (dot(high[0], both[0]) + dot(high[1], both[1])).astype(bf16))
            for value, r in zip(mixed, at):
                for h in range(4):
                    to = slice(512 * k + 128 * h, 512 * k + 128 * h + 128)
                    ctx_v[r, to] = value[128 * h : 128 * h + 128, :128]
                    tctx_v[r, to] = value[128 * h : 128 * h + 128, 128:]


def probe_kernel(place, ctx, signs, *refs):
    out = refs[-1]
    for j in range(4):
        cols = slice(512 * j, 512 * j + 512)
        value = dot(ctx[...], signs[:, cols]) * 2048 ** (-0.5)
        if len(refs) > 1:
            value += refs[0][:, cols].astype(f32)
        out[:, cols] = value.astype(bf16)


def cotangent_kernel(at, place, c0, c1, t0, t1, w, part, *refs):
    back_in, (term, back, cot) = refs[:-3], refs[-3:]
    for k in range(2):
        value = dot(t0[...], w[k, 0:1024]) + dot(t1[...], w[k, 1024:2048])
        here = slice(at + 512 * k, at + 512 * k + 512)
        cot[:, 512 * k : 512 * k + 512] = (value + part[:, here].astype(f32)).astype(bf16)
    for j, c in enumerate((c0, c1)):
        term[1024 * j : 1024 * j + 1024] = lax.dot_general(
            c[...], cot[...], ROWS, preferred_element_type=f32
        ).astype(bf16)
    for j in range(2):
        rows = slice(1024 * j, 1024 * j + 1024)
        value = lax.dot_general(cot[:, 0:512], w[0, rows], LAST, preferred_element_type=f32) + lax.dot_general(
            cot[:, 512:1024], w[1, rows], LAST, preferred_element_type=f32
        )
        if back_in:
            value += back_in[0][:, 1024 * (1 - j) : 1024 * (1 - j) + 1024].astype(f32)
        back[:, rows] = value.astype(bf16)


def value_kernel(place, n, lo0, lo1, hi0, hi1, back, own, partner, bv):
    spread = lambda p, up: lax.dot_general(p, up, ROWS, preferred_element_type=f32)
    for half, (lo, hi) in enumerate(((lo0, hi0), (lo1, hi1))):
        for k in range(2):
            at = 2 * half + k
            to = slice(128 * at, 128 * at + 128)
            for s in range(2):
                rows = (slice(SEQ * s, SEQ * s + 128), slice(SEQ * s + 128, SEQ * s + SEQ))
                head = lambda r, h: back[r, 512 * at + 128 * h : 512 * at + 128 * h + 128]
                up = [jnp.concatenate([head(r, h) for h in range(4)], 0) for r in rows]
                both = spread(hi[s, k], up[1])
                bv[rows[0], to] = (both[0:128] + spread(lo[s, k], up[0])).astype(bf16)
                bv[rows[1], to] = both[128:256].astype(bf16)
    for out, cols in ((partner, slice(256, 512)), (own, slice(0, 256))):
        out[...] = lax.dot_general(n[...], bv[:, cols], ROWS, preferred_element_type=f32).astype(bf16)


def pair_kernel(local, place, own, got, *refs):
    a, b = refs[:4], refs[4:8]
    core, y, x = place[0], place[1], place[3]
    add = lambda u, v: (u.astype(f32) + v.astype(f32)).astype(bf16)
    for by in range(4):
        row = lax.rem(y + by, 4)
        at = local_slot(row, core) if local else row
        for to in range(4):
            slot = lax.rem(x + to, 4)
            a[to][row] = add(own[at, :, slot, 0:32], got[at, :, slot, 0:32])
        b[by][...] = add(own[at, :, :, 32:64], got[at, :, :, 32:64])


def total_of(refs, index=()):
    total = refs[0][index].astype(f32)
    for r in refs[1:]:
        total += r[index].astype(f32)
    return total


def second_kernel(place, *refs):
    y, x = place[1], place[3]
    out_a, out_b = refs[16:20], refs[20:24]
    for cols, a, b in ((slice(0, 1024), refs[0:4], refs[4:8]), (slice(1024, 1280), refs[8:12], refs[12:16])):
        for by in range(4):
            out_a[by][:, :, cols] = total_of(a, lax.rem(y + by, 4)).astype(bf16)
            slot = lax.rem(x + by, 4)
            for zl in range(2):
                out_b[by][zl, :, cols] = total_of(b, (zl, slot)).astype(bf16)


def third_kernel(place, *refs):
    z = 2 * place[4] + place[2]
    a, b, out = refs[:4], refs[4:8], refs[8:]
    for by in range(4):
        to = lax.rem(z + by, 4)
        zl, zh = lax.rem(to, 2), lax.div(to, 2)
        for rows, parts in ((slice(0, 32), a), (slice(32, 64), b)):
            lo = total_of(parts, zl)
            for at, width in ((0, 512), (1024, 128)):
                left, right = lo[:, at : at + width], lo[:, at + width : at + 2 * width]
                got = jnp.where(zh == 0, left, right).astype(bf16)
                start = 0 if at == 0 else 512
                out[by][rows, start : start + width] = got


def last_kernel(place, own, before, after, across, value, output):
    total = total_of((own, before, after, across), slice(None))
    output[...] = total[:, :512]
    value[...] = total[:, 512:]


def exchanged(pieces, axis):
    return (pieces[0],) + tuple(shifted(pieces[by], axis, by) for by in (1, 3, 2))


def turn_tables():
    position = lax.broadcasted_iota(jnp.int32, (SEQ, 1), 0).astype(f32)
    exponent = lax.broadcasted_iota(jnp.int32, (1, 64), 1).astype(f32) * (-2.0 / HEAD_DIM)
    angles = position * jnp.power(f32(rope_base), exponent)
    cos, sin = jnp.cos(angles), jnp.sin(angles)
    return jnp.concatenate([cos, cos], 1), jnp.concatenate([-sin, sin], 1)


def step(hidden, norm_gain, query_weight, key_weight, value_weight, output_weight, probe_seed):
    vmem = lambda *shape: pltpu.VMEM(shape, bf16)

    a, b = call(
        cut_kernel, (query_weight, key_weight, value_weight, output_weight), [(64, 1280)] * 2,
        [dma(8)], kept=range(4), limit=60,
    )
    aq, ao, bq, bo, low_q, high_q, low_o, high_o = call(
        small_kernel, line_of(a, "x") + line_of(b, "y"),
        [(4, 64, 768), (4, 64, 512)] * 2 + [(4, 64, 768)] * 2 + [(4, 64, 512)] * 2, limit=10,
    )

    def gathered(local, a, b, low, high):
        n = a.shape[2]
        z_pair = lambda parts: (shifted(parts[0], Z, -1), shifted(parts[1], Z, 1))
        across = shifted(a, "y", 2), shifted(b, "x", 2)
        fa, fb = call(join_kernel, (a, b, *z_pair((low, high))), [(2, 4, 64, n)] * 2, limit=8)
        la = [shifted(fa, "y", by) for by in (1, -1)]
        lb = [shifted(fb, "x", by) for by in (1, -1)]
        rest = z_pair(call(split_kernel, across, [(4, 64, n)] * 2, limit=8))
        (w,) = call(
            functools.partial(order_kernel, local),
            (fa, *la, across[0], fb, *lb, across[1], *rest),
            [(2, 4, 2, 4, 64, n)], [dma(15)], far=(0,), limit=8,
        )
        return w.reshape(2, 2048, n)

    w_own = gathered(False, aq, bq, low_q, high_q)
    w_partner = shifted(w_own, "core", 1)
    o_own = gathered(True, ao, bo, low_o, high_o)
    o_partner = shifted(o_own, "core", 1)

    hidden, cos, sin = lax.optimization_barrier((hidden, *turn_tables()))
    normed, tangent_value = call(
        prepare_kernel, (hidden, norm_gain.reshape(1, 2048)), [(512, 2048), (512, 512)],
        flops=2 << 30, limit=20, seed=probe_seed,
    )
    signs0, signs1 = sign_table(probe_seed, 0), sign_table(probe_seed, 1)

    def attend(w, half):
        return call(
            functools.partial(attention_kernel, half), (normed, w, tangent_value, cos, sin),
            [(512, 1024), (512, 1024), (2, 2, 512, 128), (2, 2, 512, 256)],
            [pltpu.VMEM((2, 512, 768), f32)], flops=5 << 30, limit=LIMITS[0],
        )

    c_own, t_own, low_own, high_own = attend(w_own, 0)
    c_partner, t_partner, low_partner, high_partner = attend(w_partner, 1)
    probe = lambda *args: call(probe_kernel, args, [(512, 2048)], flops=2 << 30, limit=LIMITS[1])[0]
    part = probe(c_partner, signs1, probe(c_own, signs0))

    def cotangent(at, *args):
        return call(
            functools.partial(cotangent_kernel, at), args, [(2048, 1024), (512, 2048)],
            [vmem(512, 1024)], flops=6 << 30, limit=LIMITS[2],
        )

    term_partner, back = cotangent(1024, c_partner, c_own, t_partner, t_own, o_partner, part)
    term_own, back = cotangent(0, c_own, c_partner, t_own, t_partner, o_own, part, back)
    grid = lambda v: v.reshape(4, 2, 4, 64, v.shape[1])

    def paired(local, own, partner):
        got = shifted(partner, "core", 1)
        n = own.shape[1]
        pieces = call(
            functools.partial(pair_kernel, local), (grid(own), grid(got)),
            [(4, 2, 32, n)] * 4 + [(2, 4, 32, n)] * 4,
            limit=LIMITS[4],
        )
        return exchanged(pieces[:4], "x") + exchanged(pieces[4:], "y")

    out_pieces = paired(True, term_own, term_partner)
    val_own, val_partner = call(
        value_kernel,
        (normed, low_own, low_partner, high_own, high_partner, back), [(2048, 256)] * 2,
        [vmem(512, 512)], flops=2 << 30, limit=LIMITS[3],
    )
    val_pieces = paired(False, val_own, val_partner)
    pieces = call(second_kernel, out_pieces + val_pieces, [(2, 32, 1280)] * 8, limit=20)
    pieces = call(
        third_kernel, exchanged(pieces[:4], "y") + exchanged(pieces[4:], "x"),
        [(64, 640)] * 4, limit=8,
    )
    value, output = call(last_kernel, exchanged(pieces, Z), [(64, 128), (64, 512)], dtypes=[f32, f32], limit=4)
    return value, output


def solution(mesh):
    fine = Mesh(mesh.devices.reshape(2, 2, 4, 2, 4), AXES)
    fsdp, probe = ("y", "zl", "x"), ("zh", "core")
    return jax.shard_map(
        step,
        mesh=fine,
        in_specs=(P(AXES, None), P(), P(fsdp, None), P(fsdp, None), P(fsdp, None), P(fsdp, None), P(probe)),
        out_specs=(P(fsdp, probe), P(fsdp, probe)),
        check_vma=False,
    )
```
